128 devices in a mesh: mem: 8 (over z, x_hi), lat: 16 (over x_lo, y, core).
Axes of the slice: x: 4 (x_hi: 2, x_lo: 2; x = x_hi * 2 + x_lo), y: 4, z: 4, core: 2. Of those that a mesh axis runs over, the one named last changes fastest.
Arguments:
- features: bfloat16 [32, 32, 1440, 128], P('mem', 'lat'), may hold values from -6 to 6
- conv_inner: bfloat16 [3, 3, 128, 128], replicated, may hold values from -0.1875 to 0.1875
- conv_head: bfloat16 [3, 3, 128, 69], replicated, may hold values from -0.1875 to 0.1875
- truth: float32 [69, 32, 1440], P(None, 'lat'), may hold values from -5 to 5
- kernel_width: float32 [69], replicated, may hold values from 0.3 to 1.5
- var_weight: float32 [69], replicated, may hold values from 0.5 to 2
Outputs:
- grad_features: bfloat16 [32, 32, 1440, 128], P('mem', 'lat')
- grad_inner: float32 [3, 3, 128, 128], replicated
- grad_head: float32 [3, 3, 128, 69], replicated
The draws below stay inside these ranges and needn't reach their ends.
All inputs are finite; a program needn't handle non-finite values.
Results may differ from the reference program's by a relative error of at most 0.0098.
Values may be sent and summed in bfloat16 or wider, within the bound.
A program may use at most 256 MiB of HBM per device.

```python
import math
import jax
import jax.numpy as jnp
from jax import lax

C = 128
V = 69
LON = 1440
MEMBERS = 32
NLAT = 32


def block_scale(key, shape, pieces, smallest, high):
    factor_of, own = 1.0, jax.random.fold_in(key, 6)
    for axis_at, parts in pieces:
        steps = jnp.exp(jax.random.uniform(jax.random.fold_in(own, axis_at), (parts,), jnp.float32, smallest / len(pieces), high / len(pieces)))
        factor_of = factor_of * jnp.repeat(steps, shape[axis_at] // parts).reshape([-1 if axis == axis_at else 1 for axis in range(len(shape))])
    return factor_of


def scatter_about(own_key, dims, scale, limit, shards=(), kind=jnp.bfloat16):
    level = block_scale(own_key, dims, shards, -0.22, 0.18) if shards else 1.0
    array = jax.random.normal(own_key, dims, jnp.float32) * scale * level
    return jnp.minimum(jnp.maximum(array, -limit), limit).astype(kind)


def setup_inputs(seed: int = 0) -> dict:
    key_of = jax.random.split(jax.random.key(seed), 7)
    return {
        "features": scatter_about(key_of[0], (MEMBERS, NLAT, LON, C), 1.0, 6.0, ((0, 8), (1, 16))),
        "conv_inner": scatter_about(key_of[1], (3, 3, C, C), (9 * C) ** -0.5, 0.1875),
        "conv_head": scatter_about(key_of[2], (3, 3, C, V), (9 * C) ** -0.5, 0.1875),
        "truth": scatter_about(key_of[3], (V, NLAT, LON), 0.7, 5.0, ((1, 16),), jnp.float32),
        "kernel_width": jnp.clip(jnp.exp(jax.random.uniform(key_of[4], (V,), jnp.float32, math.log(0.3), math.log(1.5))), 0.3, 1.5),
        "var_weight": jnp.clip(jnp.exp(jax.random.uniform(key_of[5], (V,), jnp.float32, math.log(0.5), math.log(2.0))), 0.5, 2.0),
    }


def wrap_lon(values, axis):
    count = values.shape[axis]
    return jnp.concatenate([lax.slice_in_dim(values, count - 1, count, axis=axis), values, lax.slice_in_dim(values, 0, 1, axis=axis)], axis=axis)


def pad_rows(values, axis):
    widths = [(0, 0)] * values.ndim
    widths[axis] = (1, 1)
    return jnp.pad(values, widths)


def gelu_slope(pre):
    return jax.jvp(jax.nn.gelu, (pre,), (jnp.ones_like(pre),))[1]


def reference(features, conv_inner, conv_head, truth, kernel_width, var_weight):
    inner32 = conv_inner.astype(jnp.float32)
    head32 = conv_head.astype(jnp.float32)

    def forward(member):
        feature_pad = wrap_lon(pad_rows(member, 0), 1).astype(jnp.float32)
        pre = jnp.zeros((NLAT, LON, C), jnp.float32)
        for row_off in range(3):
            for col_off in range(3):
                pre = pre + jnp.einsum("rlc,co->rlo", feature_pad[row_off:row_off + NLAT, col_off:col_off + LON], inner32[row_off, col_off])
        hidden = jax.nn.gelu(pre).astype(jnp.bfloat16)
        hidden_pad = wrap_lon(pad_rows(hidden, 0), 1).astype(jnp.float32)
        field = jnp.zeros((V, NLAT, LON), jnp.float32)
        for row_off in range(3):
            for col_off in range(3):
                field = field + jnp.einsum("rlc,cv->vrl", hidden_pad[row_off:row_off + NLAT, col_off:col_off + LON], head32[row_off, col_off])
        return pre, hidden, field.astype(jnp.bfloat16)

    pres, hiddens, fields = lax.map(forward, features)
    members = features.shape[0]
    inverse = 1.0 / (kernel_width * kernel_width)
    values = fields.astype(jnp.float32)

    def variable_pairs(packed):
        member_values, rate = packed
        spread = member_values[None] - member_values[:, None]
        kernel = jnp.exp(-0.5 * spread * spread * rate)
        return jnp.sum(kernel * spread, axis=1)

    pairwise = lax.map(variable_pairs, (jnp.moveaxis(values, 1, 0), inverse))
    pairwise = jnp.moveaxis(pairwise, 0, 1)
    offset = values - truth[None]
    nearness = jnp.exp(-0.5 * offset * offset * inverse[None, :, None, None])
    scale = (var_weight * inverse)[None, :, None, None]
    field_grad = (scale * ((2.0 / (members - 1)) * pairwise + 2.0 * nearness * offset)).astype(jnp.bfloat16)

    def backward(packed):
        member, pre, hidden, grad_field = packed
        feature_pad = wrap_lon(pad_rows(member, 0), 1).astype(jnp.float32)
        hidden_pad = wrap_lon(pad_rows(hidden, 0), 1).astype(jnp.float32)
        grad_pad = wrap_lon(pad_rows(grad_field, 1), 2).astype(jnp.float32)
        grad_values = grad_field.astype(jnp.float32)
        summed = jnp.zeros((NLAT, LON, C), jnp.float32)
        head_parts = []
        for row_off in range(3):
            for col_off in range(3):
                summed = summed + jnp.einsum("vrl,cv->rlc", grad_pad[:, 2 - row_off:2 - row_off + NLAT, 2 - col_off:2 - col_off + LON], head32[row_off, col_off])
                head_parts.append(jnp.einsum("rlc,vrl->cv", hidden_pad[row_off:row_off + NLAT, col_off:col_off + LON], grad_values))
        hidden_grad = (summed * gelu_slope(pre)).astype(jnp.bfloat16)
        dpad = wrap_lon(pad_rows(hidden_grad, 0), 1).astype(jnp.float32)
        hidden_values = hidden_grad.astype(jnp.float32)
        feature_grad = jnp.zeros((NLAT, LON, C), jnp.float32)
        inner_parts = []
        for row_off in range(3):
            for col_off in range(3):
                feature_grad = feature_grad + jnp.einsum("rlo,co->rlc", dpad[2 - row_off:2 - row_off + NLAT, 2 - col_off:2 - col_off + LON], inner32[row_off, col_off])
                inner_parts.append(jnp.einsum("rlc,rlo->co", feature_pad[row_off:row_off + NLAT, col_off:col_off + LON], hidden_values))
        inner_grad = jnp.stack(inner_parts).reshape((3, 3, C, C))
        head_grad = jnp.stack(head_parts).reshape((3, 3, C, V))
        return feature_grad.astype(jnp.bfloat16), inner_grad, head_grad

    grad_features, inner_all, head_all = lax.map(backward, (features, pres, hiddens, field_grad))
    points = NLAT * LON
    return grad_features, jnp.sum(inner_all, axis=0) / points, jnp.sum(head_all, axis=0) / points
```

```python
import math
import jax
import jax.numpy as jnp
from jax import lax
from jax.experimental import pallas as pl
from jax.experimental.pallas import tpu as pltpu
from jax.sharding import PartitionSpec as P

MESH_ID = pl.DeviceIdType.MESH
F32 = jnp.float32
BF16 = jnp.bfloat16
LANE = 128
VP = 80
MEM = 8
LAT = 16
GELU_A = math.sqrt(2.0 / math.pi)
GELU_B = 0.044715


def roll_rows(values, shift):
    return pltpu.roll(values, shift % values.shape[0], 0)


def transposed(values):
    return jnp.transpose(values.astype(F32)).astype(BF16)


def whole_block(
    feat, kin, ht, prm, truth,
    gf_out, gi_out, gh_out,
    feat_rows, wide, shifted, slope, hgrad, hgrad_t, own_field,
    part_out, part_in, field_out, values_in, grad_field,
    w_inner, w_head, w_head_back, w_inner_back,
    inner_acc, head_acc, ar_in, ar_out, ar_r1, ar_r2, ar_r3, gf_buf,
    load_sem, fh_s, fh_r, ph_s, ph_r, a2_s, a2_r, b2_s, b2_r, gh_s, gh_r, hh_s, hh_r,
    r1_s, r1_r, r2_s, r2_r, r3_s, r3_r, g3_s, g3_r, g2_s, g2_r, g1_s, g1_r, out_sem,
):
    lon = feat.shape[2]
    lon_pad = grad_field.shape[3]
    members = feat.shape[0]
    third = lon_pad // 4
    d = lax.axis_index("mem")
    r = lax.axis_index("lat")
    has_up = r > 0
    has_down = r < LAT - 1
    above = lax.rem(r + LAT - 1, LAT)
    below = lax.rem(r + 1, LAT)
    half = lax.rem(r, 2)
    seat = r // 2

    def mem_peer(k):
        return lax.rem(d + k, MEM)

    def lat_peer(k):
        return lax.rem(seat + k, MEM) * 2 + half

    partner = r + 1 - 2 * half

    def remote(src, dst, ss, rs, **where):
        return pltpu.make_async_remote_copy(
            src_ref=src, dst_ref=dst, send_sem=ss, recv_sem=rs,
            device_id=where, device_id_type=MESH_ID,
        )

    barrier = pltpu.get_barrier_semaphore()
    for k in range(1, MEM):
        pl.semaphore_signal(barrier, inc=1, device_id={"mem": mem_peer(k)}, device_id_type=MESH_ID)
    for k in range(1, LAT):
        pl.semaphore_signal(
            barrier, inc=1, device_id={"lat": lax.rem(r + k, LAT)}, device_id_type=MESH_ID
        )

    def load(m, row):
        return pltpu.make_async_copy(
            feat.at[m, row], feat_rows.at[1 + row, m, pl.ds(0, lon)], load_sem.at[m, row]
        )

    for m in range(members):
        for row in range(2):
            load(m, row).start()

    pl.semaphore_wait(barrier, MEM - 1 + LAT - 1)

    def feat_halo(side, m):
        if side == 0:
            src, dst, where = feat_rows.at[1, m, pl.ds(0, lon)], feat_rows.at[3, m, pl.ds(0, lon)], above
        else:
            src, dst, where = feat_rows.at[2, m, pl.ds(0, lon)], feat_rows.at[0, m, pl.ds(0, lon)], below
        return remote(src, dst, fh_s.at[side, m], fh_r.at[side, m], lat=where)

    def part_halo(side, m):
        src = part_out.at[pl.ds(side * 4, 4), m]
        dst = part_in.at[pl.ds(side * 4, 4), m]
        return remote(src, dst, ph_s.at[side, m], ph_r.at[side, m], lat=above if side == 0 else below)

    def gfield_halo(side, m):
        if side == 0:
            src, dst, where = grad_field.at[m, 1], grad_field.at[m, 3], above
        else:
            src, dst, where = grad_field.at[m, 2], grad_field.at[m, 0], below
        return remote(src, dst, gh_s.at[side, m], gh_r.at[side, m], lat=where)

    def hgrad_halo(side, m):
        if side == 0:
            src, dst, where = hgrad.at[1, m], hgrad.at[3, m], above
        else:
            src, dst, where = hgrad.at[2, m], hgrad.at[0, m], below
        return remote(src, dst, hh_s.at[side, m], hh_r.at[side, m], lat=where)

    sides = ((0, has_up, has_down), (1, has_down, has_up))

    def send_halo(copy_of, m):
        for side, sends, _ in sides:
            @pl.when(sends)
            def _():
                copy_of(side, m).start()

    def recv_halo(copy_of, m):
        for side, _, receives in sides:
            @pl.when(receives)
            def _():
                copy_of(side, m).wait_recv()

    def drain_halo(copy_of, m):
        for side, sends, _ in sides:
            @pl.when(sends)
            def _():
                copy_of(side, m).wait_send()

    for m in range(members):
        for row in range(2):
            load(m, row).wait()
        send_halo(feat_halo, m)

    feat_rows[:, :, lon:, :] = jnp.zeros((4, members, lon_pad - lon, LANE), BF16)
    shifted[:, lon:, :] = jnp.zeros((members, lon_pad - lon, shifted.shape[2]), BF16)

    @pl.when(r == 0)
    def _():
        for m in range(members):
            feat_rows[0, m, 0:lon] = jnp.zeros((lon, LANE), BF16)
            hgrad[0, m] = jnp.zeros((lon, LANE), BF16)
            grad_field[m, 0] = jnp.zeros((VP, lon_pad), BF16)
            for q in range(4):
                part_in[4 + q, m] = jnp.zeros((VP, third), BF16)

    @pl.when(r == LAT - 1)
    def _():
        for m in range(members):
            feat_rows[3, m, 0:lon] = jnp.zeros((lon, LANE), BF16)
            hgrad[3, m] = jnp.zeros((lon, LANE), BF16)
            grad_field[m, 3] = jnp.zeros((VP, lon_pad), BF16)
            for q in range(4):
                part_in[q, m] = jnp.zeros((VP, third), BF16)

    w_inner[...] = jnp.zeros(w_inner.shape, BF16)
    w_inner_back[...] = jnp.zeros(w_inner_back.shape, BF16)
    w_head[...] = jnp.zeros(w_head.shape, BF16)
    w_head_back[...] = jnp.zeros(w_head_back.shape, BF16)
    for a in range(3):
        for b in range(3):
            block = kin[a * 3 + b]
            block_t = transposed(block)
            head_t = ht[a * 3 + b]
            for o in range(2):
                cols = slice((o * 3 + b) * LANE, (o * 3 + b + 1) * LANE)
                w_inner[(o + a) * LANE:(o + a + 1) * LANE, cols] = block
                e = o - a + 2
                w_inner_back[e * LANE:(e + 1) * LANE, cols] = block_t
                row = o - a + 2
                w_head[row * VP:(row + 1) * VP, b * 2 * LANE + o * LANE:b * 2 * LANE + (o + 1) * LANE] = head_t
            w_head_back[(2 - a) * VP:(3 - a) * VP, b * LANE:(b + 1) * LANE] = head_t

    def lanes(index):
        return slice(index * LANE, (index + 1) * LANE)

    def forward(m):
        recv_halo(feat_halo, m)
        rows = jnp.concatenate([feat_rows[e, m, 0:lon] for e in range(4)], axis=1)
        wide[...] = jnp.dot(rows, w_inner[...], preferred_element_type=F32)
        for o in range(2):
            pre = (
                roll_rows(wide[:, lanes(o * 3)], 1)
                + wide[:, lanes(o * 3 + 1)]
                + roll_rows(wide[:, lanes(o * 3 + 2)], -1)
            )
            square = pre * pre
            th = jnp.tanh(GELU_A * pre * (1.0 + GELU_B * square))
            cdf = 0.5 + 0.5 * th
            hidden = pre * cdf
            grad = cdf + 0.5 * pre * (1.0 - th * th) * (GELU_A * (1.0 + 3.0 * GELU_B * square))
            slope[m, :, lanes(o)] = grad.astype(BF16)
            shifted[m, 0:lon, lanes(o)] = roll_rows(hidden, 1).astype(BF16)
            shifted[m, 0:lon, lanes(2 + o)] = hidden.astype(BF16)
            shifted[m, 0:lon, lanes(4 + o)] = roll_rows(hidden, -1).astype(BF16)
        slot = lax.rem(m, 2)
        for q in range(4):
            sums = lax.dot_general(
                w_head[...], shifted[m, q * third:(q + 1) * third, :],
                (((1,), (1,)), ((), ())), preferred_element_type=F32,
            )
            part_out[q, m] = sums[0:VP].astype(BF16)
            own_field[slot, 0, :, q * third:(q + 1) * third] = sums[VP:2 * VP]
            own_field[slot, 1, :, q * third:(q + 1) * third] = sums[2 * VP:3 * VP]
            part_out[4 + q, m] = sums[3 * VP:4 * VP].astype(BF16)
        send_halo(part_halo, m)

    def field_copy(m, k):
        p = mem_peer(k)
        return remote(
            field_out.at[p, m], values_in.at[d, m], a2_s.at[m, k], a2_r.at[m, k], mem=p
        )

    def finish_field(m):
        recv_halo(part_halo, m)
        slot = lax.rem(m, 2)
        for row in range(2):
            for q in range(4):
                total = own_field[slot, row, :, q * third:(q + 1) * third] + part_in[
                    (1 - row) * 4 + q, m
                ].astype(F32)
                field_out[row * 4 + q, m] = total.astype(BF16)
        for k in range(1, MEM):
            field_copy(m, k).start()
        values_in[d, m] = field_out[d, m]

    def forward_step(step, carry):
        @pl.when(step < members)
        def _():
            forward(step)

        @pl.when(step > 0)
        def _():
            finish_field(step - 1)

        return carry

    lax.fori_loop(0, members + 1, forward_step, 0)

    def wait_fields(m, carry):
        for k in range(1, MEM):
            field_copy(m, k).wait()
        drain_halo(feat_halo, m)
        drain_halo(part_halo, m)
        return carry

    lax.fori_loop(0, members, wait_fields, 0)

    grad_out = field_out
    count = MEM * members
    own_row = 1 + d // 4
    own_lane = lax.rem(d, 4) * third

    def place(j):
        return slice((j // 6) * VP, (j // 6 + 1) * VP), slice((j % 6) * LANE, (j % 6 + 1) * LANE)

    def back_copy(c, k):
        p = mem_peer(k)
        return remote(
            grad_out.at[p, :, :, pl.ds(c * LANE, LANE)],
            grad_field.at[:, own_row, :, pl.ds(own_lane + c * LANE, LANE)],
            b2_s.at[c, k], b2_r.at[c, k], mem=p,
        )

    block = 8

    def pair_chunk(c, carry):
        lane = pl.ds(pl.multiple_of(c * LANE, LANE), LANE)
        scale = prm[0]
        for j in range(count):
            rows, cols = place(j)
            wide[rows, cols] = values_in[j // members, j % members, :, lane].astype(F32) * scale

        def group(g, inner):
            def at(j):
                base = (j // 6) * VP
                return pl.ds(pl.multiple_of(base + g * 8, 8), 8), slice((j % 6) * LANE, (j % 6 + 1) * LANE)

            rows8 = pl.ds(pl.multiple_of(g * 8, 8), 8)
            target = truth[rows8, lane] * prm[0, rows8]
            pair_weight = prm[1, rows8]
            truth_weight = prm[2, rows8]

            def term(x, y):
                u = x - y
                return u * jnp.exp2(u * (y - x))

            for i0 in range(0, count, block):
                xi = [wide[at(i0 + i)] for i in range(block)]
                sums = [None] * block
                for i in range(block):
                    for j in range(i + 1, block):
                        w = term(xi[j], xi[i])
                        sums[i] = w if sums[i] is None else sums[i] + w
                        sums[j] = -w if sums[j] is None else sums[j] - w
                if i0 > 0:
                    sums = [s + wide[at(count + i0 + i)] for i, s in enumerate(sums)]
                for j0 in range(i0 + block, count, 4):
                    xj = [wide[at(j0 + j)] for j in range(4)]
                    back = [None] * 4
                    for j in range(4):
                        for i in range(block):
                            w = term(xj[j], xi[i])
                            sums[i] = sums[i] + w
                            back[j] = -w if back[j] is None else back[j] - w
                    for j in range(4):
                        old = back[j] if i0 == 0 else wide[at(count + j0 + j)] + back[j]
                        wide[at(count + j0 + j)] = old
                for i in range(block):
                    near = term(xi[i], target)
                    wide[at(count + i0 + i)] = pair_weight * sums[i] + truth_weight * near
            return inner

        lax.fori_loop(0, VP // 8 - 1, group, 0)
        pad_row = jnp.zeros((VP - 72, LANE), F32)
        for j in range(count):
            rows, cols = place(count + j)
            full = jnp.concatenate([wide[rows, cols][0:72], pad_row], axis=0)
            grad_out[j // members, j % members, :, lane] = full.astype(BF16)
        for k in range(1, MEM):
            back_copy(c, k).start()
        grad_field[:, own_row, :, pl.ds(pl.multiple_of(own_lane + c * LANE, LANE), LANE)] = grad_out[d, :, :, lane]
        return carry

    chunks = third // LANE
    lax.fori_loop(0, chunks, pair_chunk, 0)

    def wait_back(c, carry):
        for k in range(1, MEM):
            back_copy(c, k).wait()
        return carry

    lax.fori_loop(0, chunks, wait_back, 0)

    for m in range(members):
        send_halo(gfield_halo, m)

    inner_acc[...] = jnp.zeros(inner_acc.shape, F32)
    head_acc[...] = jnp.zeros(head_acc.shape, F32)

    def backward(m, carry):
        recv_halo(gfield_halo, m)
        for i in range(2):
            stack = [grad_field[m, i + j] for j in range(3)]
            stack.append(jnp.zeros((2 * LANE - 3 * VP, lon_pad), BF16))
            columns = transposed(jnp.concatenate(stack, axis=0))
            wide[:, 0:3 * LANE] = jnp.dot(
                columns[0:lon], w_head_back[...], preferred_element_type=F32
            )
            total = (
                roll_rows(wide[:, lanes(0)], -1) + wide[:, lanes(1)] + roll_rows(wide[:, lanes(2)], 1)
            )
            hg = total * slope[m, :, lanes(i)].astype(F32)
            hgrad[1 + i, m] = hg.astype(BF16)
            tail = jnp.zeros((lon_pad - lon, LANE), F32)
            for b in range(3):
                moved = hg if b == 1 else roll_rows(hg, b - 1)
                hgrad_t[(i * 3 + b) * LANE:(i * 3 + b + 1) * LANE, :] = jnp.transpose(
                    jnp.concatenate([moved, tail], axis=0)
                ).astype(BF16)
        send_halo(hgrad_halo, m)
        rows = jnp.concatenate([feat_rows[e, m] for e in range(4)], axis=1)
        inner_acc[...] += jnp.dot(hgrad_t[...], rows, preferred_element_type=F32)
        fields = grad_field[m].reshape(4 * VP, lon_pad)
        head_acc[...] += jnp.dot(fields, shifted[m], preferred_element_type=F32)
        return carry

    lax.fori_loop(0, members, backward, 0)

    for a in range(3):
        for b in range(3):
            ab = a * 3 + b
            ar_in[ab * LANE:(ab + 1) * LANE] = (
                inner_acc[b * LANE:(b + 1) * LANE, lanes(a)]
                + inner_acc[(3 + b) * LANE:(4 + b) * LANE, lanes(1 + a)]
            )
            base = 9 * LANE + ab * VP
            ar_in[base:base + VP] = (
                head_acc[(2 - a) * VP:(3 - a) * VP, lanes(b * 2)]
                + head_acc[(3 - a) * VP:(4 - a) * VP, lanes(b * 2 + 1)]
            )
    used = 9 * (LANE + VP)
    total_rows = ar_in.shape[0]
    ar_in[used:] = jnp.zeros((total_rows - used, LANE), F32)
    half_rows = total_rows // 2
    mem_rows = half_rows // MEM
    seat_rows = mem_rows // MEM

    def at_rows(start, size):
        return pl.ds(pl.multiple_of(start, 8), size)

    my_half = half * half_rows
    my_mem = my_half + d * mem_rows
    my_seat = my_mem + seat * seat_rows

    def rs1():
        return remote(
            ar_in.at[at_rows((1 - half) * half_rows, half_rows)], ar_r1, r1_s, r1_r, lat=partner
        )

    def rs2(k):
        return remote(
            ar_in.at[at_rows(my_half + mem_peer(k) * mem_rows, mem_rows)],
            ar_r2.at[k], r2_s.at[k], r2_r.at[k], mem=mem_peer(k),
        )

    def rs3(k):
        return remote(
            ar_in.at[at_rows(my_mem + lax.rem(seat + k, MEM) * seat_rows, seat_rows)],
            ar_r3.at[k], r3_s.at[k], r3_r.at[k], lat=lat_peer(k),
        )

    def ag3(k):
        piece = ar_out.at[at_rows(my_seat, seat_rows)]
        return remote(piece, piece, g3_s.at[k], g3_r.at[k], lat=lat_peer(k))

    def ag2(k):
        piece = ar_out.at[at_rows(my_mem, mem_rows)]
        return remote(piece, piece, g2_s.at[k], g2_r.at[k], mem=mem_peer(k))

    def ag1():
        piece = ar_out.at[at_rows(my_half, half_rows)]
        return remote(piece, piece, g1_s, g1_r, lat=partner)

    def stage_one():
        rs1().wait()
        mine = at_rows(my_half, half_rows)
        ar_in[mine] = ar_in[mine] + ar_r1[...]
        for k in range(1, MEM):
            rs2(k).start()

    def stage_two():
        for k in range(1, MEM):
            rs2(k).wait()
        mine = at_rows(my_mem, mem_rows)
        total = ar_in[mine]
        for k in range(1, MEM):
            total = total + ar_r2[k]
        ar_in[mine] = total
        for k in range(1, MEM):
            rs3(k).start()

    def stage_three():
        for k in range(1, MEM):
            rs3(k).wait()
        mine = at_rows(my_seat, seat_rows)
        total = ar_in[mine]
        for k in range(1, MEM):
            total = total + ar_r3[k]
        ar_out[mine] = total
        for k in range(1, MEM):
            ag3(k).start()

    def gf_copy(m):
        return pltpu.make_async_copy(gf_buf.at[lax.rem(m, 2)], gf_out.at[m], out_sem.at[lax.rem(m, 2)])

    rs1().start()

    def last(m, carry):
        recv_halo(hgrad_halo, m)

        @pl.when(m >= 2)
        def _():
            gf_copy(m - 2).wait()

        rows = jnp.concatenate([hgrad[e, m] for e in range(4)], axis=1)
        wide[...] = jnp.dot(rows, w_inner_back[...], preferred_element_type=F32)
        for o in range(2):
            total = (
                roll_rows(wide[:, lanes(o * 3)], -1)
                + wide[:, lanes(o * 3 + 1)]
                + roll_rows(wide[:, lanes(o * 3 + 2)], 1)
            )
            gf_buf[lax.rem(m, 2), o] = total.astype(BF16)
        gf_copy(m).start()

        @pl.when(m == 0)
        def _():
            stage_one()

        @pl.when(m == 1)
        def _():
            stage_two()

        @pl.when(m == 2)
        def _():
            stage_three()

        return carry

    lax.fori_loop(0, members, last, 0)

    for k in range(1, MEM):
        ag3(k).wait()
    for k in range(1, MEM):
        ag2(k).start()
    for m in range(members):
        drain_halo(gfield_halo, m)
        drain_halo(hgrad_halo, m)
    for k in range(1, MEM):
        ag2(k).wait()
    ag1().start()
    for m in range(max(members - 2, 0), members):
        gf_copy(m).wait()
    ag1().wait()

    points = 1.0 / (2 * LAT * lon)
    variables = gh_out.shape[2]
    for ab in range(9):
        gi_out[ab] = jnp.transpose(ar_out[ab * LANE:(ab + 1) * LANE]) * points
        base = 9 * LANE + ab * VP
        piece = jnp.concatenate(
            [ar_out[base:base + VP], jnp.zeros((LANE - VP, LANE), F32)], axis=0
        )
        gh_out[ab] = (jnp.transpose(piece) * points)[:, 0:variables]


def shards(features, conv_inner, conv_head, truth, kernel_width, var_weight):
    members, band, lon, channels = features.shape
    variables = conv_head.shape[3]
    lon_pad = -(-lon // (4 * LANE)) * 4 * LANE
    third = lon_pad // 4
    kin = conv_inner.reshape(9, channels, channels)
    ht = jnp.pad(
        jnp.swapaxes(conv_head.reshape(9, channels, variables), 1, 2),
        ((0, 0), (0, VP - variables), (0, 0)),
    )
    inverse = 1.0 / (kernel_width * kernel_width)
    scale = jnp.sqrt(0.5 * math.log2(math.e) * inverse)
    weight = var_weight * inverse / scale
    total_members = members * lax.axis_size("mem")
    prm = jnp.stack([scale, weight * (2.0 / (total_members - 1)), weight * 2.0])
    prm = jnp.broadcast_to(
        jnp.pad(prm, ((0, 0), (0, VP - variables)))[:, :, None], (3, VP, LANE)
    )
    d = lax.axis_index("mem")
    padded = jnp.pad(truth, ((0, VP - variables), (0, 0), (0, lon_pad - lon)))
    piece = lax.dynamic_slice(
        padded, (0, d // 4, lax.rem(d, 4) * third), (VP, 1, third)
    ).reshape(VP, third)

    any_spec = pl.BlockSpec(memory_space=pl.ANY)
    vmem = pl.BlockSpec(memory_space=pltpu.VMEM)
    dma = pltpu.SemaphoreType.DMA
    total_rows = 2048
    scratch = [
        pltpu.VMEM((4, members, lon_pad, LANE), BF16),
        pltpu.VMEM((lon, 6 * LANE), F32),
        pltpu.VMEM((members, lon_pad, 6 * LANE), BF16),
        pltpu.VMEM((members, lon, 2 * LANE), BF16),
        pltpu.VMEM((4, members, lon, LANE), BF16),
        pltpu.VMEM((6 * LANE, lon_pad), BF16),
        pltpu.VMEM((2, 2, VP, lon_pad), F32),
        pltpu.VMEM((MEM, members, VP, third), BF16),
        pltpu.VMEM((MEM, members, VP, third), BF16),
        pltpu.VMEM((MEM, members, VP, third), BF16),
        pltpu.VMEM((MEM, members, VP, third), BF16),
        pltpu.VMEM((members, 4, VP, lon_pad), BF16),
        pltpu.VMEM((4 * LANE, 6 * LANE), BF16),
        pltpu.VMEM((4 * VP, 6 * LANE), BF16),
        pltpu.VMEM((2 * LANE, 3 * LANE), BF16),
        pltpu.VMEM((4 * LANE, 6 * LANE), BF16),
        pltpu.VMEM((6 * LANE, 4 * LANE), F32),
        pltpu.VMEM((4 * VP, 6 * LANE), F32),
        pltpu.VMEM((total_rows, LANE), F32),
        pltpu.VMEM((total_rows, LANE), F32),
        pltpu.VMEM((total_rows // 2, LANE), F32),
        pltpu.VMEM((MEM, total_rows // 2 // MEM, LANE), F32),
        pltpu.VMEM((MEM, total_rows // 2 // MEM // MEM, LANE), F32),
        pltpu.VMEM((2, 2, lon, LANE), BF16),
        dma((members, 2)),
        dma((2, members)), dma((2, members)),
        dma((2, members)), dma((2, members)),
        dma((members, MEM)), dma((members, MEM)),
        dma((third // LANE, MEM)), dma((third // LANE, MEM)),
        dma((2, members)), dma((2, members)),
        dma((2, members)), dma((2, members)),
        dma, dma,
        dma((MEM,)), dma((MEM,)),
        dma((MEM,)), dma((MEM,)),
        dma((MEM,)), dma((MEM,)),
        dma((MEM,)), dma((MEM,)),
        dma, dma,
        dma((2,)),
    ]
    grad_features, inner, head = pl.pallas_call(
        whole_block,
        out_shape=(
            jax.ShapeDtypeStruct(features.shape, BF16),
            jax.ShapeDtypeStruct((9, channels, channels), F32),
            jax.ShapeDtypeStruct((9, channels, variables), F32),
        ),
        in_specs=[any_spec, vmem, vmem, vmem, vmem],
        out_specs=(any_spec, vmem, vmem),
        scratch_shapes=scratch,
        compiler_params=pltpu.CompilerParams(
            collective_id=0, has_side_effects=True, vmem_limit_bytes=67043328
        ),
    )(features, kin, ht, prm, piece)
    return (
        grad_features,
        inner.reshape(3, 3, channels, channels),
        head.reshape(3, 3, channels, variables),
    )


def solution(mesh):
    in_specs = (P("mem", "lat", None, None), P(), P(), P(None, "lat", None), P(), P())
    out_specs = (P("mem", "lat", None, None), P(), P())
    return jax.shard_map(shards, mesh=mesh, in_specs=in_specs, out_specs=out_specs, check_vma=False)
```

```python
import math
import jax
import jax.numpy as jnp
from jax import lax
from jax.experimental import pallas as pl
from jax.experimental.pallas import tpu as pltpu
from jax.sharding import PartitionSpec as P

MESH_ID = pl.DeviceIdType.MESH
F32 = jnp.float32
BF16 = jnp.bfloat16
LANE = 128
VP = 80
MEM = 8
LAT = 16
HEAD_ROWS = 768
RELAYS = (0, LAT - 1)
GELU_A = math.sqrt(2.0 / math.pi)
GELU_B = 0.044715


def roll_rows(values, shift):
    return pltpu.roll(values, shift % values.shape[0], 0)


def transposed(values):
    return jnp.transpose(values.astype(F32)).astype(BF16)


def whole_block(
    feat, kin, ht, width, weight, truth,
    gf_out, gi_out, gh_out,
    feat_rows, wide, shifted, slope, hgrad, hgrad_t, own_field,
    part_out, part_in, field_out, values_in, grad_field,
    w_inner, w_head, w_head_back, w_inner_back,
    feat_relay, part_relay, gfield_relay, hgrad_relay,
    inner_acc, head_acc, gf_buf, prm, target_buf,
    hs_in, hs_out, hs_r1, hs_r2, hs_r3, is_in, is_out, is_r1, is_r2, is_r3,
    load_sem, fh_s, fh_r, ph_s, ph_r, a2_s, a2_r, b2_s, b2_r, gh_s, gh_r, hh_s, hh_r,
    hsum_sems, isum_sems, out_sem, relay_s, relay_r,
):
    lon = feat.shape[2]
    lon_pad = grad_field.shape[3]
    members = feat.shape[0]
    third = lon_pad // 4
    d = lax.axis_index("mem")
    r = lax.axis_index("lat")
    has_up = r > 0
    has_down = r < LAT - 1
    above = lax.rem(r + LAT - 1, LAT)
    below = lax.rem(r + 1, LAT)
    half = lax.rem(r, 2)
    seat = r // 2

    def mem_peer(k):
        return lax.rem(d + k, MEM)

    def lat_peer(k):
        return lax.rem(seat + k, MEM) * 2 + half

    partner = r + 1 - 2 * half

    def remote(src, dst, ss, rs, **where):
        return pltpu.make_async_remote_copy(
            src_ref=src, dst_ref=dst, send_sem=ss, recv_sem=rs,
            device_id=where, device_id_type=MESH_ID,
        )

    barrier = pltpu.get_barrier_semaphore()
    for k in range(1, MEM):
        pl.semaphore_signal(barrier, inc=1, device_id={"mem": mem_peer(k)}, device_id_type=MESH_ID)
    for k in range(1, LAT):
        pl.semaphore_signal(
            barrier, inc=1, device_id={"lat": lax.rem(r + k, LAT)}, device_id_type=MESH_ID
        )

    def load(m, row):
        return pltpu.make_async_copy(
            feat.at[m, row], feat_rows.at[1 + row, m, pl.ds(0, lon)], load_sem.at[m, row]
        )

    for m in range(members):
        for row in range(2):
            load(m, row).start()

    pl.semaphore_wait(barrier, MEM - 1 + LAT - 1)

    mid_up = r == LAT // 2 - 1
    mid_down = r == LAT // 2
    relay_down = RELAYS[0]
    relay_up = RELAYS[1]
    is_relay = jnp.logical_or(r == relay_down, r == relay_up)
    relay_end = jnp.where(r == relay_down, LAT // 2, LAT // 2 - 1)
    part_rows = lon // 2

    def halo_rows(part):
        return pl.ds(part * part_rows, part_rows)

    def feat_ends(side, part, m):
        own, other = (1, 3) if side == 0 else (2, 0)
        return feat_rows.at[own, m, halo_rows(part)], feat_rows.at[other, m, halo_rows(part)]

    def part_ends(side, part, m):
        slots = pl.ds(side * 4 + part * 2, 2)
        return part_out.at[slots, m], part_in.at[slots, m]

    def gfield_ends(side, part, t):
        own, other = (1, 3) if side == 0 else (2, 0)
        rows = pl.ds(pl.multiple_of(t * 16, 16), 16)
        half_members = pl.ds(part * (members // 2), members // 2)
        return grad_field.at[half_members, own, rows], grad_field.at[half_members, other, rows]

    def hgrad_ends(side, part, m):
        own, other = (1, 3) if side == 0 else (2, 0)
        return hgrad.at[own, m, halo_rows(part)], hgrad.at[other, m, halo_rows(part)]

    feat_halo = (feat_ends, fh_s, fh_r, feat_relay, 0)
    part_halo = (part_ends, ph_s, ph_r, part_relay, 1)
    gfield_halo = (gfield_ends, gh_s, gh_r, gfield_relay, 2)
    hgrad_halo = (hgrad_ends, hh_s, hh_r, hgrad_relay, 3)

    sides = (
        (0, has_up, has_down, above, mid_down, relay_up),
        (1, has_down, has_up, below, mid_up, relay_down),
    )

    def direct(kind, side, part, m, where):
        ends, ss, rs, _, _ = kind
        src, dst = ends(side, part, m)
        return remote(src, dst, ss.at[side * 2 + part, m], rs.at[side * 2 + part, m], lat=where)

    def to_relay(kind, side, m, where):
        ends, ss, _, buffer, row = kind
        return remote(ends(side, 1, m)[0], buffer.at[m], ss.at[side * 2 + 1, m], relay_r.at[row, m], lat=where)

    def from_relay(kind, side, m):
        ends, _, rs, buffer, row = kind
        return remote(
            buffer.at[m], ends(side, 1, m)[1], relay_s.at[row, m], rs.at[side * 2 + 1, m], lat=relay_end
        )

    def send_halo(kind, m):
        for side, sends, _, where, by_relay, relay in sides:
            @pl.when(jnp.logical_and(sends, jnp.logical_not(by_relay)))
            def _():
                direct(kind, side, 0, m, where).start()
                direct(kind, side, 1, m, where).start()

            @pl.when(by_relay)
            def _():
                to_relay(kind, side, m, relay).start()
                direct(kind, side, 0, m, where).start()

    def recv_halo(kind, m):
        for side, _, receives, where, _, _ in sides:
            @pl.when(receives)
            def _():
                direct(kind, side, 0, m, where).wait_recv()
                direct(kind, side, 1, m, where).wait_recv()

    def drain_halo(kind, m):
        for side, sends, _, where, _, _ in sides:
            @pl.when(sends)
            def _():
                direct(kind, side, 0, m, where).wait_send()
                direct(kind, side, 1, m, where).wait_send()

        for side, relay in ((0, relay_up), (1, relay_down)):
            @pl.when(r == relay)
            def _():
                from_relay(kind, side, m).wait_send()

    def pass_on(kind, m):
        for side, relay in ((0, relay_up), (1, relay_down)):
            @pl.when(r == relay)
            def _():
                to_relay(kind, side, m, relay_end).wait_recv()
                from_relay(kind, side, m).start()

    for m in range(members):
        for row in range(2):
            load(m, row).wait()
        send_halo(feat_halo, m)

    feat_rows[:, :, lon:, :] = jnp.zeros((4, members, lon_pad - lon, LANE), BF16)
    shifted[:, lon:, :] = jnp.zeros((members, lon_pad - lon, shifted.shape[2]), BF16)

    @pl.when(r == 0)
    def _():
        for m in range(members):
            feat_rows[0, m, 0:lon] = jnp.zeros((lon, LANE), BF16)
            hgrad[0, m] = jnp.zeros((lon, LANE), BF16)
            grad_field[m, 0] = jnp.zeros((VP, lon_pad), BF16)
            for q in range(4):
                part_in[4 + q, m] = jnp.zeros((VP, third), BF16)

    @pl.when(r == LAT - 1)
    def _():
        for m in range(members):
            feat_rows[3, m, 0:lon] = jnp.zeros((lon, LANE), BF16)
            hgrad[3, m] = jnp.zeros((lon, LANE), BF16)
            grad_field[m, 3] = jnp.zeros((VP, lon_pad), BF16)
            for q in range(4):
                part_in[q, m] = jnp.zeros((VP, third), BF16)

    w_inner[...] = jnp.zeros(w_inner.shape, BF16)
    w_inner_back[...] = jnp.zeros(w_inner_back.shape, BF16)
    w_head[...] = jnp.zeros(w_head.shape, BF16)
    w_head_back[...] = jnp.zeros(w_head_back.shape, BF16)
    for a in range(3):
        for b in range(3):
            block = kin[a * 3 + b]
            block_t = transposed(block)
            head_t = ht[a * 3 + b]
            nv = head_t.shape[0]
            for o in range(2):
                cols = slice((o * 3 + b) * LANE, (o * 3 + b + 1) * LANE)
                w_inner[(o + a) * LANE:(o + a + 1) * LANE, cols] = block
                e = o - a + 2
                w_inner_back[e * LANE:(e + 1) * LANE, cols] = block_t
                row = o - a + 2
                w_head[row * VP:row * VP + nv, b * 2 * LANE + o * LANE:b * 2 * LANE + (o + 1) * LANE] = head_t
            w_head_back[(2 - a) * VP:(2 - a) * VP + nv, b * LANE:(b + 1) * LANE] = head_t

    def column(ref, fill):
        nv = ref.shape[1]
        row = jnp.concatenate([ref[...], jnp.full((1, LANE - nv), fill, F32)], axis=1)
        return jnp.transpose(jnp.broadcast_to(row, (LANE, LANE)))[0:VP]

    widths = column(width, 1.0)
    inverse = 1.0 / (widths * widths)
    scaling = jnp.sqrt(0.5 * math.log2(math.e) * inverse)
    factor = column(weight, 0.0) * inverse / scaling
    prm[0] = scaling
    prm[1] = factor * (2.0 / (MEM * members - 1))
    prm[2] = factor * 2.0
    target_buf[...] = jnp.zeros(target_buf.shape, F32)
    for quarter in range(4):
        for row in range(2):
            @pl.when(d == row * 4 + quarter)
            def _():
                stop = min((quarter + 1) * third, lon)
                target_buf[0:truth.shape[0], 0:stop - quarter * third] = truth[:, row, quarter * third:stop]

    def lanes(index):
        return slice(index * LANE, (index + 1) * LANE)

    def forward(m):
        recv_halo(feat_halo, m)
        rows = jnp.concatenate([feat_rows[e, m, 0:lon] for e in range(4)], axis=1)
        wide[...] = jnp.dot(rows, w_inner[...], preferred_element_type=F32)
        for o in range(2):
            pre = (
                roll_rows(wide[:, lanes(o * 3)], 1)
                + wide[:, lanes(o * 3 + 1)]
                + roll_rows(wide[:, lanes(o * 3 + 2)], -1)
            )
            square = pre * pre
            th = jnp.tanh(GELU_A * pre * (1.0 + GELU_B * square))
            cdf = 0.5 + 0.5 * th
            hidden = pre * cdf
            grad = cdf + 0.5 * pre * (1.0 - th * th) * (GELU_A * (1.0 + 3.0 * GELU_B * square))
            slope[m, :, lanes(o)] = grad.astype(BF16)
            shifted[m, 0:lon, lanes(o)] = roll_rows(hidden, 1).astype(BF16)
            shifted[m, 0:lon, lanes(2 + o)] = hidden.astype(BF16)
            shifted[m, 0:lon, lanes(4 + o)] = roll_rows(hidden, -1).astype(BF16)
        slot = m
        for q in range(4):
            sums = lax.dot_general(
                w_head[...], shifted[m, q * third:(q + 1) * third, :],
                (((1,), (1,)), ((), ())), preferred_element_type=F32,
            )
            part_out[q, m] = sums[0:VP].astype(BF16)
            own_field[slot, 0, :, q * third:(q + 1) * third] = sums[VP:2 * VP]
            own_field[slot, 1, :, q * third:(q + 1) * third] = sums[2 * VP:3 * VP]
            part_out[4 + q, m] = sums[3 * VP:4 * VP].astype(BF16)
        send_halo(part_halo, m)

    chunks = VP // 16

    def tile(t):
        return pl.ds(t * 16 if isinstance(t, int) else pl.multiple_of(t * 16, 16), 16)

    def field_copy(m, t, k):
        p = mem_peer(k)
        return remote(
            field_out.at[p, m, tile(t)], values_in.at[d, m, tile(t)],
            a2_s.at[m * chunks + t, k], a2_r.at[m * chunks + t, k], mem=p,
        )

    def finish_field(m):
        recv_halo(part_halo, m)
        slot = m
        for row in range(2):
            for q in range(4):
                total = own_field[slot, row, :, q * third:(q + 1) * third] + part_in[
                    (1 - row) * 4 + q, m
                ].astype(F32)
                field_out[row * 4 + q, m] = total.astype(BF16)
        for t in range(chunks):
            for k in range(1, MEM):
                field_copy(m, t, k).start()
        values_in[d, m] = field_out[d, m]

    for m in range(members):
        pass_on(feat_halo, m)

    def forward_step(m, carry):
        forward(m)

        @pl.when(m > 0)
        def _():
            pass_on(part_halo, m - 1)

        return carry

    def finish_step(m, carry):
        finish_field(m)
        return carry

    lax.fori_loop(0, members, forward_step, 0)
    pass_on(part_halo, members - 1)
    lax.fori_loop(0, members, finish_step, 0)

    grad_out = field_out
    count = MEM * members
    own_row = 1 + d // 4
    own_lane = lax.rem(d, 4) * third

    def place(j):
        return slice((j // 2) * 16, (j // 2 + 1) * 16), slice((j % 2) * third, (j % 2 + 1) * third)

    def back_copy(t, k):
        p = mem_peer(k)
        rows = tile(t)
        return remote(
            grad_out.at[p, :, rows],
            grad_field.at[:, own_row, rows, pl.ds(pl.multiple_of(own_lane, LANE), third)],
            b2_s.at[t, k], b2_r.at[t, k], mem=p,
        )

    block = 8
    lane_groups = third // LANE
    used_groups = -(-truth.shape[0] // 8)

    def pair_chunk(t, carry):
        rows16 = tile(t)

        def arrived(m, inner):
            for k in range(1, MEM):
                field_copy(m, t, k).wait()
            return inner

        lax.fori_loop(0, members, arrived, 0)
        scale = jnp.concatenate([prm[0, rows16]] * lane_groups, axis=1)
        for j in range(count):
            rows, cols = place(j)
            wide[rows, cols] = values_in[j // members, j % members, rows16].astype(F32) * scale

        def group(unit, inner):
            sub = unit // lane_groups
            lane = lax.rem(unit, lane_groups) * LANE

            def at(j):
                return (
                    pl.ds(pl.multiple_of((j // 2) * 16 + sub * 8, 8), 8),
                    pl.ds(pl.multiple_of((j % 2) * third + lane, LANE), LANE),
                )

            rows8 = pl.ds(pl.multiple_of(t * 16 + sub * 8, 8), 8)
            target = target_buf[rows8, pl.ds(pl.multiple_of(lane, LANE), LANE)] * prm[0, rows8]
            pair_weight = prm[1, rows8]
            truth_weight = prm[2, rows8]

            def term(x, y):
                u = x - y
                return u * jnp.exp2(u * (y - x))

            for i0 in range(0, count, block):
                xi = [wide[at(i0 + i)] for i in range(block)]
                sums = [None] * block
                for i in range(block):
                    for j in range(i + 1, block):
                        w = term(xi[j], xi[i])
                        sums[i] = w if sums[i] is None else sums[i] + w
                        sums[j] = -w if sums[j] is None else sums[j] - w
                if i0 > 0:
                    sums = [s + wide[at(count + i0 + i)] for i, s in enumerate(sums)]
                for j0 in range(i0 + block, count, 4):
                    xj = [wide[at(j0 + j)] for j in range(4)]
                    back = [None] * 4
                    for j in range(4):
                        for i in range(block):
                            w = term(xj[j], xi[i])
                            sums[i] = sums[i] + w
                            back[j] = -w if back[j] is None else back[j] - w
                    for j in range(4):
                        old = back[j] if i0 == 0 else wide[at(count + j0 + j)] + back[j]
                        wide[at(count + j0 + j)] = old
                for i in range(block):
                    near = term(xi[i], target)
                    wide[at(count + i0 + i)] = pair_weight * sums[i] + truth_weight * near
            return inner

        subs = jnp.minimum(2, used_groups - 2 * t)
        lax.fori_loop(0, subs * lane_groups, group, 0)
        keep = lax.broadcasted_iota(jnp.int32, (16, third), 0) < subs * 8
        for j in range(count):
            rows, cols = place(count + j)
            grad_out[j // members, j % members, rows16] = jnp.where(keep, wide[rows, cols], 0.0).astype(BF16)
        for k in range(1, MEM):
            back_copy(t, k).start()
        grad_field[:, own_row, rows16, pl.ds(pl.multiple_of(own_lane, LANE), third)] = grad_out[d, :, rows16]
        return carry

    lax.fori_loop(0, chunks, pair_chunk, 0)

    def wait_back(t, carry):
        for k in range(1, MEM):
            back_copy(t, k).wait()
        send_halo(gfield_halo, t)
        return carry

    lax.fori_loop(0, chunks, wait_back, 0)

    inner_acc[...] = jnp.zeros(inner_acc.shape, F32)
    head_acc[...] = jnp.zeros(head_acc.shape, F32)

    def at_rows(start, size):
        return pl.ds(pl.multiple_of(start, 8), size)

    def device_sum(src, dst, r1, r2, r3, sems):
        half_rows = src.shape[0] // 2
        piece_rows = half_rows // MEM
        my_half = half * half_rows
        my_piece = my_half + d * piece_rows
        s1, s2, s3, s4, s5 = [(sems.at[2 * n], sems.at[2 * n + 1]) for n in range(5)]

        def scatter_pair():
            return remote(
                src.at[at_rows((1 - half) * half_rows, half_rows)], r1, s1[0].at[0], s1[1].at[0], lat=partner
            )

        def scatter(k):
            return remote(
                src.at[at_rows(my_half + mem_peer(k) * piece_rows, piece_rows)],
                r2.at[k], s2[0].at[k], s2[1].at[k], mem=mem_peer(k),
            )

        def share(k):
            return remote(src.at[at_rows(my_piece, piece_rows)], r3.at[seat], s3[0].at[k], s3[1].at[k], lat=lat_peer(k))

        def gather(k):
            piece = dst.at[at_rows(my_piece, piece_rows)]
            return remote(piece, piece, s4[0].at[k], s4[1].at[k], mem=mem_peer(k))

        def gather_pair():
            piece = dst.at[at_rows(my_half, half_rows)]
            return remote(piece, piece, s5[0].at[0], s5[1].at[0], lat=partner)

        def each(copy_of, act):
            for k in range(1, MEM):
                act(copy_of(k))

        start = lambda c: c.start()
        wait = lambda c: c.wait()

        def step_0():
            scatter_pair().start()

        def step_1():
            scatter_pair().wait()
            mine = at_rows(my_half, half_rows)
            src[mine] = src[mine] + r1[...]
            each(scatter, start)

        def step_2():
            each(scatter, wait)
            mine = at_rows(my_piece, piece_rows)
            total = src[mine]
            for k in range(1, MEM):
                total = total + r2[k]
            src[mine] = total
            each(share, start)
            r3[seat] = total

        def step_3():
            each(share, wait)
            total = r3[0]
            for k in range(1, MEM):
                total = total + r3[k]
            dst[at_rows(my_piece, piece_rows)] = total * (1.0 / (2 * LAT * lon))
            each(gather, start)

        def step_4():
            each(gather, wait)
            gather_pair().start()

        def step_5():
            gather_pair().wait()

        return step_0, step_1, step_2, step_3, step_4, step_5

    head_steps = device_sum(hs_in, hs_out, hs_r1, hs_r2, hs_r3, hsum_sems)
    inner_steps = device_sum(is_in, is_out, is_r1, is_r2, is_r3, isum_sems)

    def head_gradient(m, carry):
        fields = grad_field[m].reshape(4 * VP, lon_pad)
        head_acc[...] += jnp.dot(fields, shifted[m], preferred_element_type=F32)
        return carry

    def halo_tiles(t, carry):
        pass_on(gfield_halo, t)
        recv_halo(gfield_halo, t)
        return carry

    lax.fori_loop(0, chunks, halo_tiles, 0)
    lax.fori_loop(0, members, head_gradient, 0)
    for a in range(3):
        for b in range(3):
            base = (a * 3 + b) * VP
            hs_in[base:base + VP] = (
                head_acc[(2 - a) * VP:(3 - a) * VP, lanes(b * 2)]
                + head_acc[(3 - a) * VP:(4 - a) * VP, lanes(b * 2 + 1)]
            )
    hs_in[9 * VP:] = jnp.zeros((hs_in.shape[0] - 9 * VP, LANE), F32)
    head_steps[0]()

    def backward(m, carry):
        for i in range(2):
            stack = [grad_field[m, i + j] for j in range(3)]
            stack.append(jnp.zeros((2 * LANE - 3 * VP, lon_pad), BF16))
            columns = transposed(jnp.concatenate(stack, axis=0))
            wide[:, 0:3 * LANE] = jnp.dot(
                columns[0:lon], w_head_back[...], preferred_element_type=F32
            )
            total = (
                roll_rows(wide[:, lanes(0)], -1) + wide[:, lanes(1)] + roll_rows(wide[:, lanes(2)], 1)
            )
            hg = total * slope[m, :, lanes(i)].astype(F32)
            hgrad[1 + i, m] = hg.astype(BF16)
            tail = jnp.zeros((lon_pad - lon, LANE), F32)
            for b in range(3):
                moved = hg if b == 1 else roll_rows(hg, b - 1)
                hgrad_t[(i * 3 + b) * LANE:(i * 3 + b + 1) * LANE, :] = jnp.transpose(
                    jnp.concatenate([moved, tail], axis=0)
                ).astype(BF16)
        send_halo(hgrad_halo, m)
        rows = jnp.concatenate([feat_rows[e, m] for e in range(4)], axis=1)
        inner_acc[...] += jnp.dot(hgrad_t[...], rows, preferred_element_type=F32)
        @pl.when(m >= 1)
        def _():
            pass_on(hgrad_halo, m - 1)

        @pl.when(m == 1)
        def _():
            head_steps[1]()

        return carry

    lax.fori_loop(0, members, backward, 0)
    for a in range(3):
        for b in range(3):
            ab = a * 3 + b
            is_in[ab * LANE:(ab + 1) * LANE] = jnp.transpose(
                inner_acc[b * LANE:(b + 1) * LANE, lanes(a)]
                + inner_acc[(3 + b) * LANE:(4 + b) * LANE, lanes(1 + a)]
            )

    def gf_copy(m):
        return pltpu.make_async_copy(gf_buf.at[lax.rem(m, 2)], gf_out.at[m], out_sem.at[lax.rem(m, 2)])

    inner_steps[0]()
    pass_on(hgrad_halo, members - 1)

    def last(m, carry):
        recv_halo(hgrad_halo, m)

        @pl.when(m >= 2)
        def _():
            gf_copy(m - 2).wait()

        rows = jnp.concatenate([hgrad[e, m] for e in range(4)], axis=1)
        wide[...] = jnp.dot(rows, w_inner_back[...], preferred_element_type=F32)
        for o in range(2):
            total = (
                roll_rows(wide[:, lanes(o * 3)], -1)
                + wide[:, lanes(o * 3 + 1)]
                + roll_rows(wide[:, lanes(o * 3 + 2)], 1)
            )
            gf_buf[lax.rem(m, 2), o] = total.astype(BF16)
        gf_copy(m).start()

        for n in range(members):
            @pl.when(m == n)
            def _():
                if n > 0:
                    head_steps[n + 1]()
                inner_steps[n + 1]()

        return carry

    lax.fori_loop(0, members, last, 0)

    for m in range(members):
        drain_halo(feat_halo, m)
        drain_halo(part_halo, m)
        drain_halo(hgrad_halo, m)
    for t in range(chunks):
        drain_halo(gfield_halo, t)
    for m in range(max(members - 2, 0), members):
        gf_copy(m).wait()
    head_steps[5]()
    for ab in range(9):
        gh_out[ab] = hs_out[ab * VP:ab * VP + gh_out.shape[1]]
    inner_steps[5]()
    for ab in range(9):
        gi_out[ab] = is_out[ab * LANE:(ab + 1) * LANE]


def sum_scratch(rows):
    piece = rows // 2 // MEM
    return [
        pltpu.VMEM((rows, LANE), F32),
        pltpu.VMEM((rows, LANE), F32),
        pltpu.VMEM((rows // 2, LANE), F32),
        pltpu.VMEM((MEM, piece, LANE), F32),
        pltpu.VMEM((MEM, piece, LANE), F32),
    ]


def shards(features, conv_inner, conv_head, truth, kernel_width, var_weight):
    members, band, lon, channels = features.shape
    variables = conv_head.shape[3]
    lon_pad = -(-lon // (4 * LANE)) * 4 * LANE
    third = lon_pad // 4
    kin = conv_inner.reshape(9, channels, channels)
    ht = jnp.swapaxes(conv_head.reshape(9, channels, variables), 1, 2)
    width = kernel_width.reshape(1, variables)
    weight = var_weight.reshape(1, variables)

    any_spec = pl.BlockSpec(memory_space=pl.ANY)
    vmem = pl.BlockSpec(memory_space=pltpu.VMEM)
    dma = pltpu.SemaphoreType.DMA
    scratch = [
        pltpu.VMEM((4, members, lon_pad, LANE), BF16),
        pltpu.VMEM((lon, 6 * LANE), F32),
        pltpu.VMEM((members, lon_pad, 6 * LANE), BF16),
        pltpu.VMEM((members, lon, 2 * LANE), BF16),
        pltpu.VMEM((4, members, lon, LANE), BF16),
        pltpu.VMEM((6 * LANE, lon_pad), BF16),
        pltpu.VMEM((members, 2, VP, lon_pad), F32),
        pltpu.VMEM((MEM, members, VP, third), BF16),
        pltpu.VMEM((MEM, members, VP, third), BF16),
        pltpu.VMEM((MEM, members, VP, third), BF16),
        pltpu.VMEM((MEM, members, VP, third), BF16),
        pltpu.VMEM((members, 4, VP, lon_pad), BF16),
        pltpu.VMEM((4 * LANE, 6 * LANE), BF16),
        pltpu.VMEM((4 * VP, 6 * LANE), BF16),
        pltpu.VMEM((2 * LANE, 3 * LANE), BF16),
        pltpu.VMEM((4 * LANE, 6 * LANE), BF16),
        pltpu.VMEM((members, lon // 2, LANE), BF16),
        pltpu.VMEM((members, 2, VP, third), BF16),
        pltpu.VMEM((VP // 16, members // 2, 16, lon_pad), BF16),
        pltpu.VMEM((members, lon // 2, LANE), BF16),
        pltpu.VMEM((6 * LANE, 4 * LANE), F32),
        pltpu.VMEM((4 * VP, 6 * LANE), F32),
        pltpu.VMEM((2, 2, lon, LANE), BF16),
        pltpu.VMEM((3, VP, LANE), F32),
        pltpu.VMEM((VP, third), F32),
        *sum_scratch(HEAD_ROWS),
        *sum_scratch(9 * LANE),
        dma((members, 2)),
        dma((4, members)), dma((4, members)),
        dma((4, members)), dma((4, members)),
        dma((members * VP // 16, MEM)), dma((members * VP // 16, MEM)),
        dma((VP // 16, MEM)), dma((VP // 16, MEM)),
        dma((4, VP // 16)), dma((4, VP // 16)),
        dma((4, members)), dma((4, members)),
        dma((10, MEM)), dma((10, MEM)),
        dma((2,)),
        dma((4, VP // 16)), dma((4, VP // 16)),
    ]
    grad_features, inner, head = pl.pallas_call(
        whole_block,
        out_shape=(
            jax.ShapeDtypeStruct(features.shape, BF16),
            jax.ShapeDtypeStruct((9, channels, channels), F32),
            jax.ShapeDtypeStruct((9, variables, channels), F32),
        ),
        in_specs=[any_spec, vmem, vmem, vmem, vmem, vmem],
        out_specs=(any_spec, vmem, vmem),
        scratch_shapes=scratch,
        compiler_params=pltpu.CompilerParams(
            collective_id=0, has_side_effects=True, vmem_limit_bytes=67043328
        ),
    )(features, kin, ht, width, weight, truth)
    return (
        grad_features,
        inner.reshape(3, 3, channels, channels),
        jnp.swapaxes(head, 1, 2).reshape(3, 3, channels, variables),
    )


def solution(mesh):
    in_specs = (P("mem", "lat", None, None), P(), P(), P(None, "lat", None), P(), P())
    out_specs = (P("mem", "lat", None, None), P(), P())
    return jax.shard_map(shards, mesh=mesh, in_specs=in_specs, out_specs=out_specs, check_vma=False)
```

```python
import math
import jax
import jax.numpy as jnp
from jax import lax
from jax.experimental import pallas as pl
from jax.experimental.pallas import tpu as pltpu
from jax.sharding import PartitionSpec as P

MESH_ID = pl.DeviceIdType.MESH
F32 = jnp.float32
BF16 = jnp.bfloat16
LANE = 128
VP = 80
MEM = 8
LAT = 16
HEAD_ROWS = 768
RELAYS = (0, LAT - 1)
GELU_A = math.sqrt(2.0 / math.pi)
GELU_B = 0.044715


def roll_rows(values, shift):
    return pltpu.roll(values, shift % values.shape[0], 0)


def transposed(values):
    return jnp.transpose(values.astype(F32)).astype(BF16)


def whole_block(
    feat, kin, ht, width, weight, truth,
    gf_out, gi_out, gh_out,
    feat_rows, wide, shifted, slope, hgrad, hgrad_t, own_field,
    part_out, part_in, field_out, values_in, grad_field,
    w_inner, w_head, w_head_back, w_inner_back,
    feat_relay, part_relay, gfield_relay, hgrad_relay,
    inner_acc, head_acc, gf_buf, prm, target_buf,
    hs_in, hs_out, hs_r1, hs_r2, hs_r3, is_in, is_out, is_r1, is_r2, is_r3,
    load_sem, fh_s, fh_r, ph_s, ph_r, a2_s, a2_r, b2_s, b2_r, gh_s, gh_r, hh_s, hh_r,
    hsum_sems, isum_sems, out_sem, relay_s, relay_r,
):
    lon = feat.shape[2]
    lon_pad = grad_field.shape[3]
    members = feat.shape[0]
    third = lon_pad // 4
    d = lax.axis_index("mem")
    r = lax.axis_index("lat")
    has_up = r > 0
    has_down = r < LAT - 1
    above = lax.rem(r + LAT - 1, LAT)
    below = lax.rem(r + 1, LAT)
    half = lax.rem(r, 2)
    seat = r // 2

    def mem_peer(k):
        return lax.rem(d + k, MEM)

    def lat_peer(k):
        return lax.rem(seat + k, MEM) * 2 + half

    partner = r + 1 - 2 * half

    def remote(src, dst, ss, rs, **where):
        return pltpu.make_async_remote_copy(
            src_ref=src, dst_ref=dst, send_sem=ss, recv_sem=rs,
            device_id=where, device_id_type=MESH_ID,
        )

    barrier = pltpu.get_barrier_semaphore()
    for k in range(1, MEM):
        pl.semaphore_signal(barrier, inc=1, device_id={"mem": mem_peer(k)}, device_id_type=MESH_ID)
    for k in range(1, LAT):
        pl.semaphore_signal(
            barrier, inc=1, device_id={"lat": lax.rem(r + k, LAT)}, device_id_type=MESH_ID
        )

    def load(m, row):
        return pltpu.make_async_copy(
            feat.at[m, row], feat_rows.at[1 + row, m, pl.ds(0, lon)], load_sem.at[m]
        )

    for m in range(members):
        for row in range(2):
            load(m, row).start()

    pl.semaphore_wait(barrier, MEM - 1 + LAT - 1)

    mid_up = r == LAT // 2 - 1
    mid_down = r == LAT // 2
    relay_down = RELAYS[0]
    relay_up = RELAYS[1]
    is_relay = jnp.logical_or(r == relay_down, r == relay_up)
    relay_end = jnp.where(r == relay_down, LAT // 2, LAT // 2 - 1)
    part_rows = lon // 2

    def halo_rows(part):
        return pl.ds(0, lon) if part is None else pl.ds(part * part_rows, part_rows)

    def feat_ends(side, part, m):
        own, other = (1, 3) if side == 0 else (2, 0)
        return feat_rows.at[own, m, halo_rows(part)], feat_rows.at[other, m, halo_rows(part)]

    def part_ends(side, part, m):
        slots = pl.ds(side * 4, 4) if part is None else pl.ds(side * 4 + part * 2, 2)
        return part_out.at[slots, m], part_in.at[slots, m]

    def gfield_ends(side, part, t):
        own, other = (1, 3) if side == 0 else (2, 0)
        rows = pl.ds(pl.multiple_of(t * 16, 16), 16)
        which = pl.ds(0, members) if part is None else pl.ds(part * (members // 2), members // 2)
        return grad_field.at[which, own, rows], grad_field.at[which, other, rows]

    def hgrad_ends(side, part, m):
        own, other = (1, 3) if side == 0 else (2, 0)
        return hgrad.at[own, m, halo_rows(part)], hgrad.at[other, m, halo_rows(part)]

    feat_halo = (feat_ends, fh_s, fh_r, feat_relay, 0)
    part_halo = (part_ends, ph_s, ph_r, part_relay, 1)
    gfield_halo = (gfield_ends, gh_s, gh_r, gfield_relay, 2)
    hgrad_halo = (hgrad_ends, hh_s, hh_r, hgrad_relay, 3)

    sides = (
        (0, has_up, has_down, above, mid_down, relay_up),
        (1, has_down, has_up, below, mid_up, relay_down),
    )

    def direct(kind, side, part, m, where):
        ends, ss, rs, _, _ = kind
        src, dst = ends(side, part, m)
        return remote(src, dst, ss.at[side, m], rs.at[side, m], lat=where)

    def to_relay(kind, side, m, where):
        ends, ss, _, buffer, row = kind
        return remote(ends(side, 1, m)[0], buffer.at[m], ss.at[side, m], relay_r.at[row, m], lat=where)

    def from_relay(kind, side, m):
        ends, _, rs, buffer, row = kind
        return remote(
            buffer.at[m], ends(side, 1, m)[1], relay_s.at[row, m], rs.at[side, m], lat=relay_end
        )

    def send_halo(kind, m):
        for side, sends, _, where, by_relay, relay in sides:
            @pl.when(jnp.logical_and(sends, jnp.logical_not(by_relay)))
            def _():
                direct(kind, side, 0, m, where).start()
                direct(kind, side, 1, m, where).start()

            @pl.when(by_relay)
            def _():
                to_relay(kind, side, m, relay).start()
                direct(kind, side, 0, m, where).start()

    def recv_halo(kind, m):
        for side, _, receives, where, _, _ in sides:
            @pl.when(receives)
            def _():
                direct(kind, side, None, m, where).wait_recv()

    def drain_halo(kind, m):
        for side, sends, _, where, _, _ in sides:
            @pl.when(sends)
            def _():
                direct(kind, side, None, m, where).wait_send()

        for side, relay in ((0, relay_up), (1, relay_down)):
            @pl.when(r == relay)
            def _():
                from_relay(kind, side, m).wait_send()

    def pass_on(kind, m):
        for side, relay in ((0, relay_up), (1, relay_down)):
            @pl.when(r == relay)
            def _():
                to_relay(kind, side, m, relay_end).wait_recv()
                from_relay(kind, side, m).start()

    for m in range(members):
        pltpu.make_async_copy(
            feat.at[m], feat_rows.at[pl.ds(1, 2), m, pl.ds(0, lon)], load_sem.at[m]
        ).wait()
        send_halo(feat_halo, m)

    feat_rows[:, :, lon:, :] = jnp.zeros((4, members, lon_pad - lon, LANE), BF16)
    shifted[:, lon:, :] = jnp.zeros((members, lon_pad - lon, shifted.shape[2]), BF16)

    @pl.when(r == 0)
    def _():
        for m in range(members):
            feat_rows[0, m, 0:lon] = jnp.zeros((lon, LANE), BF16)
            hgrad[0, m] = jnp.zeros((lon, LANE), BF16)
            grad_field[m, 0] = jnp.zeros((VP, lon_pad), BF16)
            for q in range(4):
                part_in[4 + q, m] = jnp.zeros((VP, third), BF16)

    @pl.when(r == LAT - 1)
    def _():
        for m in range(members):
            feat_rows[3, m, 0:lon] = jnp.zeros((lon, LANE), BF16)
            hgrad[3, m] = jnp.zeros((lon, LANE), BF16)
            grad_field[m, 3] = jnp.zeros((VP, lon_pad), BF16)
            for q in range(4):
                part_in[q, m] = jnp.zeros((VP, third), BF16)

    w_inner[...] = jnp.zeros(w_inner.shape, BF16)
    w_inner_back[...] = jnp.zeros(w_inner_back.shape, BF16)
    w_head[...] = jnp.zeros(w_head.shape, BF16)
    w_head_back[...] = jnp.zeros(w_head_back.shape, BF16)
    for a in range(3):
        for b in range(3):
            block = kin[a * 3 + b]
            block_t = transposed(block)
            head_t = ht[a * 3 + b]
            nv = head_t.shape[0]
            for o in range(2):
                cols = slice((o * 3 + b) * LANE, (o * 3 + b + 1) * LANE)
                w_inner[(o + a) * LANE:(o + a + 1) * LANE, cols] = block
                e = o - a + 2
                w_inner_back[e * LANE:(e + 1) * LANE, cols] = block_t
                row = o - a + 2
                w_head[row * VP:row * VP + nv, b * 2 * LANE + o * LANE:b * 2 * LANE + (o + 1) * LANE] = head_t
            w_head_back[(2 - a) * VP:(2 - a) * VP + nv, b * LANE:(b + 1) * LANE] = head_t

    def column(ref, fill):
        nv = ref.shape[1]
        row = jnp.concatenate([ref[...], jnp.full((1, LANE - nv), fill, F32)], axis=1)
        return jnp.transpose(jnp.broadcast_to(row, (LANE, LANE)))[0:VP]

    widths = column(width, 1.0)
    inverse = 1.0 / (widths * widths)
    scaling = jnp.sqrt(0.5 * math.log2(math.e) * inverse)
    factor = column(weight, 0.0) * inverse / scaling
    prm[0] = scaling
    prm[1] = factor * (2.0 / (MEM * members - 1))
    prm[2] = factor * 2.0
    target_buf[...] = jnp.zeros(target_buf.shape, F32)
    for quarter in range(4):
        for row in range(2):
            @pl.when(d == row * 4 + quarter)
            def _():
                stop = min((quarter + 1) * third, lon)
                target_buf[0:truth.shape[0], 0:stop - quarter * third] = truth[:, row, quarter * third:stop]

    def lanes(index):
        return slice(index * LANE, (index + 1) * LANE)

    def forward(m):
        recv_halo(feat_halo, m)
        rows = jnp.concatenate([feat_rows[e, m, 0:lon] for e in range(4)], axis=1)
        wide[...] = jnp.dot(rows, w_inner[...], preferred_element_type=F32)
        for o in range(2):
            pre = (
                roll_rows(wide[:, lanes(o * 3)], 1)
                + wide[:, lanes(o * 3 + 1)]
                + roll_rows(wide[:, lanes(o * 3 + 2)], -1)
            )
            square = pre * pre
            th = jnp.tanh(GELU_A * pre * (1.0 + GELU_B * square))
            cdf = 0.5 + 0.5 * th
            hidden = pre * cdf
            grad = cdf + 0.5 * pre * (1.0 - th * th) * (GELU_A * (1.0 + 3.0 * GELU_B * square))
            slope[m, :, lanes(o)] = grad.astype(BF16)
            shifted[m, 0:lon, lanes(o)] = roll_rows(hidden, 1).astype(BF16)
            shifted[m, 0:lon, lanes(2 + o)] = hidden.astype(BF16)
            shifted[m, 0:lon, lanes(4 + o)] = roll_rows(hidden, -1).astype(BF16)
        slot = m
        for q in range(4):
            sums = lax.dot_general(
                w_head[...], shifted[m, q * third:(q + 1) * third, :],
                (((1,), (1,)), ((), ())), preferred_element_type=F32,
            )
            part_out[q, m] = sums[0:VP].astype(BF16)
            own_field[slot, 0, :, q * third:(q + 1) * third] = sums[VP:2 * VP]
            own_field[slot, 1, :, q * third:(q + 1) * third] = sums[2 * VP:3 * VP]
            part_out[4 + q, m] = sums[3 * VP:4 * VP].astype(BF16)
        send_halo(part_halo, m)

    chunks = VP // 16

    def tile(t):
        return pl.ds(t * 16 if isinstance(t, int) else pl.multiple_of(t * 16, 16), 16)

    def field_copy(m, t, k):
        p = mem_peer(k)
        return remote(
            field_out.at[p, m, tile(t)], values_in.at[d, m, tile(t)],
            a2_s.at[t], a2_r.at[t], mem=p,
        )

    def finish_field(m):
        recv_halo(part_halo, m)
        slot = m
        for row in range(2):
            for q in range(4):
                total = own_field[slot, row, :, q * third:(q + 1) * third] + part_in[
                    (1 - row) * 4 + q, m
                ].astype(F32)
                field_out[row * 4 + q, m] = total.astype(BF16)
        for t in range(chunks):
            for k in range(1, MEM):
                field_copy(m, t, k).start()
        values_in[d, m] = field_out[d, m]

    pass_on(feat_halo, 0)
    pass_on(feat_halo, 1)

    def forward_step(m, carry):
        forward(m)

        @pl.when(m == 0)
        def _():
            for n in range(2, members):
                pass_on(feat_halo, n)

        @pl.when(m > 0)
        def _():
            pass_on(part_halo, m - 1)

        return carry

    def finish_step(m, carry):
        finish_field(m)
        return carry

    lax.fori_loop(0, members, forward_step, 0)
    pass_on(part_halo, members - 1)
    lax.fori_loop(0, members, finish_step, 0)

    grad_out = field_out
    count = MEM * members
    own_row = 1 + d // 4
    own_lane = lax.rem(d, 4) * third

    def place(j):
        return slice((j // 2) * 16, (j // 2 + 1) * 16), slice((j % 2) * third, (j % 2 + 1) * third)

    def back_copy(t, k):
        p = mem_peer(k)
        rows = tile(t)
        return remote(
            grad_out.at[p, :, rows],
            grad_field.at[:, own_row, rows, pl.ds(pl.multiple_of(own_lane, LANE), third)],
            b2_s.at[t], b2_r.at[t], mem=p,
        )

    block = 8
    lane_groups = third // LANE
    used_groups = -(-truth.shape[0] // 8)

    def pair_chunk(t, carry):
        rows16 = tile(t)

        others = pl.ds(0, MEM - 1)
        remote(
            field_out.at[others, :, rows16], values_in.at[others, :, rows16],
            a2_s.at[t], a2_r.at[t], mem=mem_peer(1),
        ).wait()
        scale = jnp.concatenate([prm[0, rows16]] * lane_groups, axis=1)
        for j in range(count):
            rows, cols = place(j)
            wide[rows, cols] = values_in[j // members, j % members, rows16].astype(F32) * scale

        def group(unit, inner):
            sub = unit // lane_groups
            lane = lax.rem(unit, lane_groups) * LANE

            def at(j):
                return (
                    pl.ds(pl.multiple_of((j // 2) * 16 + sub * 8, 8), 8),
                    pl.ds(pl.multiple_of((j % 2) * third + lane, LANE), LANE),
                )

            rows8 = pl.ds(pl.multiple_of(t * 16 + sub * 8, 8), 8)
            target = target_buf[rows8, pl.ds(pl.multiple_of(lane, LANE), LANE)] * prm[0, rows8]
            pair_weight = prm[1, rows8]
            truth_weight = prm[2, rows8]

            def term(x, y):
                u = x - y
                return u * jnp.exp2(u * (y - x))

            for i0 in range(0, count, block):
                xi = [wide[at(i0 + i)] for i in range(block)]
                sums = [None] * block
                for i in range(block):
                    for j in range(i + 1, block):
                        w = term(xi[j], xi[i])
                        sums[i] = w if sums[i] is None else sums[i] + w
                        sums[j] = -w if sums[j] is None else sums[j] - w
                if i0 > 0:
                    sums = [s + wide[at(count + i0 + i)] for i, s in enumerate(sums)]
                for j0 in range(i0 + block, count, 4):
                    xj = [wide[at(j0 + j)] for j in range(4)]
                    back = [None] * 4
                    for j in range(4):
                        for i in range(block):
                            w = term(xj[j], xi[i])
                            sums[i] = sums[i] + w
                            back[j] = -w if back[j] is None else back[j] - w
                    for j in range(4):
                        old = back[j] if i0 == 0 else wide[at(count + j0 + j)] + back[j]
                        wide[at(count + j0 + j)] = old
                for i in range(block):
                    near = term(xi[i], target)
                    wide[at(count + i0 + i)] = pair_weight * sums[i] + truth_weight * near
            return inner

        subs = jnp.minimum(2, used_groups - 2 * t)
        lax.fori_loop(0, subs * lane_groups, group, 0)
        keep = lax.broadcasted_iota(jnp.int32, (16, third), 0) < subs * 8
        for j in range(count):
            rows, cols = place(count + j)
            grad_out[j // members, j % members, rows16] = jnp.where(keep, wide[rows, cols], 0.0).astype(BF16)
        for k in range(1, MEM):
            back_copy(t, k).start()
        grad_field[:, own_row, rows16, pl.ds(pl.multiple_of(own_lane, LANE), third)] = grad_out[d, :, rows16]
        return carry

    lax.fori_loop(0, chunks, pair_chunk, 0)

    def wait_back(t, carry):
        others = pl.ds(0, MEM - 1)
        remote(
            grad_out.at[others, :, tile(t)], values_in.at[others, :, tile(t)],
            b2_s.at[t], b2_r.at[t], mem=mem_peer(1),
        ).wait()
        send_halo(gfield_halo, t)

        @pl.when(t > 0)
        def _():
            pass_on(gfield_halo, t - 1)

        return carry

    lax.fori_loop(0, chunks, wait_back, 0)

    inner_acc[...] = jnp.zeros(inner_acc.shape, F32)
    head_acc[...] = jnp.zeros(head_acc.shape, F32)

    def at_rows(start, size):
        return pl.ds(pl.multiple_of(start, 8), size)

    def device_sum(src, dst, r1, r2, r3, sems):
        half_rows = src.shape[0] // 2
        piece_rows = half_rows // MEM
        my_half = half * half_rows
        my_piece = my_half + d * piece_rows

        def scatter_pair():
            return remote(
                src.at[at_rows((1 - half) * half_rows, half_rows)], r1, sems.at[0], sems.at[1], lat=partner
            )

        def scatter(k):
            return remote(
                src.at[at_rows(my_half + mem_peer(k) * piece_rows, piece_rows)],
                r2.at[k], sems.at[2], sems.at[3], mem=mem_peer(k),
            )

        def share(k):
            return remote(src.at[at_rows(my_piece, piece_rows)], r3.at[seat], sems.at[4], sems.at[5], lat=lat_peer(k))

        def gather(k):
            piece = dst.at[at_rows(my_piece, piece_rows)]
            return remote(piece, piece, sems.at[6], sems.at[7], mem=mem_peer(k))

        def gather_pair():
            piece = dst.at[at_rows(my_half, half_rows)]
            return remote(piece, piece, sems.at[8], sems.at[9], lat=partner)

        def each(copy_of, act):
            for k in range(1, MEM):
                act(copy_of(k))

        start = lambda c: c.start()

        def wait_all(n, where):
            size = (MEM - 1) * piece_rows
            remote(
                src.at[pl.ds(0, size)], dst.at[pl.ds(0, size)], sems.at[2 * n], sems.at[2 * n + 1], **where
            ).wait()

        def step_0():
            scatter_pair().start()

        def step_1():
            scatter_pair().wait()
            mine = at_rows(my_half, half_rows)
            src[mine] = src[mine] + r1[...]
            each(scatter, start)

        def step_2():
            wait_all(1, {"mem": mem_peer(1)})
            mine = at_rows(my_piece, piece_rows)
            total = src[mine]
            for k in range(1, MEM):
                total = total + r2[k]
            src[mine] = total
            each(share, start)
            r3[seat] = total

        def step_3():
            wait_all(2, {"lat": lat_peer(1)})
            total = r3[0]
            for k in range(1, MEM):
                total = total + r3[k]
            dst[at_rows(my_piece, piece_rows)] = total * (1.0 / (2 * LAT * lon))
            each(gather, start)

        def step_4():
            wait_all(3, {"mem": mem_peer(1)})
            gather_pair().start()

        def step_5():
            gather_pair().wait()

        return step_0, step_1, step_2, step_3, step_4, step_5

    head_steps = device_sum(hs_in, hs_out, hs_r1, hs_r2, hs_r3, hsum_sems)
    inner_steps = device_sum(is_in, is_out, is_r1, is_r2, is_r3, isum_sems)

    def head_gradient(m, carry):
        fields = grad_field[m].reshape(4 * VP, lon_pad)
        head_acc[...] += jnp.dot(fields, shifted[m], preferred_element_type=F32)
        return carry

    def halo_tiles(t, carry):
        recv_halo(gfield_halo, t)
        return carry

    pass_on(gfield_halo, chunks - 1)
    lax.fori_loop(0, chunks, halo_tiles, 0)
    lax.fori_loop(0, members, head_gradient, 0)
    for a in range(3):
        for b in range(3):
            base = (a * 3 + b) * VP
            hs_in[base:base + VP] = (
                head_acc[(2 - a) * VP:(3 - a) * VP, lanes(b * 2)]
                + head_acc[(3 - a) * VP:(4 - a) * VP, lanes(b * 2 + 1)]
            )
    hs_in[9 * VP:] = jnp.zeros((hs_in.shape[0] - 9 * VP, LANE), F32)
    head_steps[0]()

    def backward(m, carry):
        for i in range(2):
            stack = [grad_field[m, i + j] for j in range(3)]
            stack.append(jnp.zeros((2 * LANE - 3 * VP, lon_pad), BF16))
            columns = transposed(jnp.concatenate(stack, axis=0))
            wide[:, 0:3 * LANE] = jnp.dot(
                columns[0:lon], w_head_back[...], preferred_element_type=F32
            )
            total = (
                roll_rows(wide[:, lanes(0)], -1) + wide[:, lanes(1)] + roll_rows(wide[:, lanes(2)], 1)
            )
            hg = total * slope[m, :, lanes(i)].astype(F32)
            hgrad[1 + i, m] = hg.astype(BF16)
            tail = jnp.zeros((lon_pad - lon, LANE), F32)
            for b in range(3):
                moved = hg if b == 1 else roll_rows(hg, b - 1)
                hgrad_t[(i * 3 + b) * LANE:(i * 3 + b + 1) * LANE, :] = jnp.transpose(
                    jnp.concatenate([moved, tail], axis=0)
                ).astype(BF16)
        send_halo(hgrad_halo, m)
        rows = jnp.concatenate([feat_rows[e, m] for e in range(4)], axis=1)
        inner_acc[...] += jnp.dot(hgrad_t[...], rows, preferred_element_type=F32)
        @pl.when(m >= 1)
        def _():
            pass_on(hgrad_halo, m - 1)

        @pl.when(m == 1)
        def _():
            head_steps[1]()

        return carry

    lax.fori_loop(0, members, backward, 0)
    for a in range(3):
        for b in range(3):
            ab = a * 3 + b
            is_in[ab * LANE:(ab + 1) * LANE] = jnp.transpose(
                inner_acc[b * LANE:(b + 1) * LANE, lanes(a)]
                + inner_acc[(3 + b) * LANE:(4 + b) * LANE, lanes(1 + a)]
            )

    def gf_copy(m):
        return pltpu.make_async_copy(gf_buf.at[lax.rem(m, 2)], gf_out.at[m], out_sem.at[lax.rem(m, 2)])

    inner_steps[0]()

    def last(m, carry):
        recv_halo(hgrad_halo, m)

        @pl.when(m >= 2)
        def _():
            gf_copy(m - 2).wait()

        rows = jnp.concatenate([hgrad[e, m] for e in range(4)], axis=1)
        wide[...] = jnp.dot(rows, w_inner_back[...], preferred_element_type=F32)
        for o in range(2):
            total = (
                roll_rows(wide[:, lanes(o * 3)], -1)
                + wide[:, lanes(o * 3 + 1)]
                + roll_rows(wide[:, lanes(o * 3 + 2)], 1)
            )
            gf_buf[lax.rem(m, 2), o] = total.astype(BF16)
        gf_copy(m).start()

        for n in range(members):
            @pl.when(m == n)
            def _():
                if n > 0:
                    head_steps[n + 1]()
                inner_steps[n + 1]()
                if n == 0:
                    pass_on(hgrad_halo, members - 1)

        return carry

    lax.fori_loop(0, members, last, 0)

    for m in range(members):
        drain_halo(feat_halo, m)
        drain_halo(part_halo, m)
        drain_halo(hgrad_halo, m)
    for t in range(chunks):
        drain_halo(gfield_halo, t)
    for m in range(max(members - 2, 0), members):
        gf_copy(m).wait()
    head_steps[5]()
    for ab in range(9):
        gh_out[ab] = hs_out[ab * VP:ab * VP + gh_out.shape[1]]
    inner_steps[5]()
    for ab in range(9):
        gi_out[ab] = is_out[ab * LANE:(ab + 1) * LANE]


def sum_scratch(rows):
    piece = rows // 2 // MEM
    return [
        pltpu.VMEM((rows, LANE), F32),
        pltpu.VMEM((rows, LANE), F32),
        pltpu.VMEM((rows // 2, LANE), F32),
        pltpu.VMEM((MEM, piece, LANE), F32),
        pltpu.VMEM((MEM, piece, LANE), F32),
    ]


def shards(features, conv_inner, conv_head, truth, kernel_width, var_weight):
    members, band, lon, channels = features.shape
    variables = conv_head.shape[3]
    lon_pad = -(-lon // (4 * LANE)) * 4 * LANE
    third = lon_pad // 4
    kin = conv_inner.reshape(9, channels, channels)
    ht = jnp.swapaxes(conv_head.reshape(9, channels, variables), 1, 2)
    width = kernel_width.reshape(1, variables)
    weight = var_weight.reshape(1, variables)

    any_spec = pl.BlockSpec(memory_space=pl.ANY)
    vmem = pl.BlockSpec(memory_space=pltpu.VMEM)
    dma = pltpu.SemaphoreType.DMA
    scratch = [
        pltpu.VMEM((4, members, lon_pad, LANE), BF16),
        pltpu.VMEM((lon, 6 * LANE), F32),
        pltpu.VMEM((members, lon_pad, 6 * LANE), BF16),
        pltpu.VMEM((members, lon, 2 * LANE), BF16),
        pltpu.VMEM((4, members, lon, LANE), BF16),
        pltpu.VMEM((6 * LANE, lon_pad), BF16),
        pltpu.VMEM((members, 2, VP, lon_pad), F32),
        pltpu.VMEM((MEM, members, VP, third), BF16),
        pltpu.VMEM((MEM, members, VP, third), BF16),
        pltpu.VMEM((MEM, members, VP, third), BF16),
        pltpu.VMEM((MEM, members, VP, third), BF16),
        pltpu.VMEM((members, 4, VP, lon_pad), BF16),
        pltpu.VMEM((4 * LANE, 6 * LANE), BF16),
        pltpu.VMEM((4 * VP, 6 * LANE), BF16),
        pltpu.VMEM((2 * LANE, 3 * LANE), BF16),
        pltpu.VMEM((4 * LANE, 6 * LANE), BF16),
        pltpu.VMEM((members, lon // 2, LANE), BF16),
        pltpu.VMEM((members, 2, VP, third), BF16),
        pltpu.VMEM((VP // 16, members // 2, 16, lon_pad), BF16),
        pltpu.VMEM((members, lon // 2, LANE), BF16),
        pltpu.VMEM((6 * LANE, 4 * LANE), F32),
        pltpu.VMEM((4 * VP, 6 * LANE), F32),
        pltpu.VMEM((2, 2, lon, LANE), BF16),
        pltpu.VMEM((3, VP, LANE), F32),
        pltpu.VMEM((VP, third), F32),
        *sum_scratch(HEAD_ROWS),
        *sum_scratch(9 * LANE),
        dma((members,)),
        dma((2, members)), dma((2, members)),
        dma((2, members)), dma((2, members)),
        dma((VP // 16,)), dma((VP // 16,)),
        dma((VP // 16,)), dma((VP // 16,)),
        dma((2, VP // 16)), dma((2, VP // 16)),
        dma((2, members)), dma((2, members)),
        dma((10,)), dma((10,)),
        dma((2,)),
        dma((4, VP // 16)), dma((4, VP // 16)),
    ]
    grad_features, inner, head = pl.pallas_call(
        whole_block,
        out_shape=(
            jax.ShapeDtypeStruct(features.shape, BF16),
            jax.ShapeDtypeStruct((9, channels, channels), F32),
            jax.ShapeDtypeStruct((9, variables, channels), F32),
        ),
        in_specs=[any_spec, vmem, vmem, vmem, vmem, vmem],
        out_specs=(any_spec, vmem, vmem),
        scratch_shapes=scratch,
        compiler_params=pltpu.CompilerParams(
            collective_id=0, has_side_effects=True, vmem_limit_bytes=67043328
        ),
    )(features, kin, ht, width, weight, truth)
    return (
        grad_features,
        inner.reshape(3, 3, channels, channels),
        jnp.swapaxes(head, 1, 2).reshape(3, 3, channels, variables),
    )


def solution(mesh):
    in_specs = (P("mem", "lat", None, None), P(), P(), P(None, "lat", None), P(), P())
    out_specs = (P("mem", "lat", None, None), P(), P())
    return jax.shard_map(shards, mesh=mesh, in_specs=in_specs, out_specs=out_specs, check_vma=False)
```

```python
import math
import jax
import jax.numpy as jnp
from jax import lax
from jax.experimental import pallas as pl
from jax.experimental.pallas import tpu as pltpu
from jax.sharding import PartitionSpec as P

MESH_ID = pl.DeviceIdType.MESH
F32 = jnp.float32
BF16 = jnp.bfloat16
LANE = 128
VP = 80
MEM = 8
LAT = 16
HEAD_ROWS = 768
RELAYS = (0, LAT - 1)
GELU_A = math.sqrt(2.0 / math.pi)
GELU_B = 0.044715


def roll_rows(values, shift):
    return pltpu.roll(values, shift % values.shape[0], 0)


def transposed(values):
    return jnp.transpose(values.astype(F32)).astype(BF16)


def whole_block(
    feat, kin, ht, width, weight, truth,
    gf_out, gi_out, gh_out,
    feat_rows, wide, shifted, slope, hgrad, hgrad_t, own_field,
    part_out, part_in, field_out, values_in, grad_field,
    w_inner, w_head, w_head_back, w_inner_back,
    feat_relay, part_relay, gfield_relay, hgrad_relay,
    inner_acc, head_acc, gf_buf, prm, target_buf,
    hs_in, hs_out, hs_r1, hs_r2, hs_r3, hs_sb, hs_db,
    is_in, is_out, is_r1, is_r2, is_r3, is_sb, is_db,
    load_sem, fh_s, fh_r, ph_s, ph_r, a2_s, a2_r, b2_s, b2_r, gh_s, gh_r, hh_s, hh_r,
    hsum_sems, isum_sems, out_sem, relay_s, relay_r,
):
    lon = feat.shape[2]
    lon_pad = grad_field.shape[3]
    members = feat.shape[0]
    third = lon_pad // 4
    d = lax.axis_index("mem")
    r = lax.axis_index("lat")
    has_up = r > 0
    has_down = r < LAT - 1
    above = lax.rem(r + LAT - 1, LAT)
    below = lax.rem(r + 1, LAT)
    half = lax.rem(r, 2)
    seat = r // 2

    def mem_peer(k):
        return lax.rem(d + k, MEM)

    def lat_peer(k):
        return lax.rem(seat + k, MEM) * 2 + half

    partner = r + 1 - 2 * half

    def remote(src, dst, ss, rs, **where):
        return pltpu.make_async_remote_copy(
            src_ref=src, dst_ref=dst, send_sem=ss, recv_sem=rs,
            device_id=where, device_id_type=MESH_ID,
        )

    barrier = pltpu.get_barrier_semaphore()
    for k in range(1, MEM):
        pl.semaphore_signal(barrier, inc=1, device_id={"mem": mem_peer(k)}, device_id_type=MESH_ID)
    for k in range(1, LAT):
        pl.semaphore_signal(
            barrier, inc=1, device_id={"lat": lax.rem(r + k, LAT)}, device_id_type=MESH_ID
        )

    def load(m, row):
        return pltpu.make_async_copy(
            feat.at[m, row], feat_rows.at[1 + row, m, pl.ds(0, lon)], load_sem.at[m]
        )

    for m in range(members):
        for row in range(2):
            load(m, row).start()

    pl.semaphore_wait(barrier, MEM - 1 + LAT - 1)

    mid_up = r == LAT // 2 - 1
    mid_down = r == LAT // 2
    relay_down = RELAYS[0]
    relay_up = RELAYS[1]
    is_relay = jnp.logical_or(r == relay_down, r == relay_up)
    relay_end = jnp.where(r == relay_down, LAT // 2, LAT // 2 - 1)
    part_rows = lon // 2

    def halo_rows(part):
        return pl.ds(0, lon) if part is None else pl.ds(part * part_rows, part_rows)

    def feat_ends(side, part, m):
        own, other = (1, 3) if side == 0 else (2, 0)
        return feat_rows.at[own, m, halo_rows(part)], feat_rows.at[other, m, halo_rows(part)]

    def part_ends(side, part, m):
        slots = pl.ds(side * 4, 4) if part is None else pl.ds(side * 4 + part * 2, 2)
        return part_out.at[slots, m], part_in.at[slots, m]

    def gfield_ends(side, part, t):
        own, other = (1, 3) if side == 0 else (2, 0)
        rows = pl.ds(pl.multiple_of(t * 16, 16), 16)
        which = pl.ds(0, members) if part is None else pl.ds(part * (members // 2), members // 2)
        return grad_field.at[which, own, rows], grad_field.at[which, other, rows]

    def hgrad_ends(side, part, m):
        own, other = (1, 3) if side == 0 else (2, 0)
        return hgrad.at[own, m, halo_rows(part)], hgrad.at[other, m, halo_rows(part)]

    feat_halo = (feat_ends, fh_s, fh_r, feat_relay, 0)
    part_halo = (part_ends, ph_s, ph_r, part_relay, 1)
    gfield_halo = (gfield_ends, gh_s, gh_r, gfield_relay, 2)
    hgrad_halo = (hgrad_ends, hh_s, hh_r, hgrad_relay, 3)

    sides = (
        (0, has_up, has_down, above, mid_down, relay_up),
        (1, has_down, has_up, below, mid_up, relay_down),
    )

    def direct(kind, side, part, m, where):
        ends, ss, rs, _, _ = kind
        src, dst = ends(side, part, m)
        return remote(src, dst, ss.at[side, m], rs.at[side, m], lat=where)

    def to_relay(kind, side, m, where):
        ends, ss, _, buffer, row = kind
        return remote(ends(side, 1, m)[0], buffer.at[m], ss.at[side, m], relay_r.at[row, m], lat=where)

    def from_relay(kind, side, m):
        ends, _, rs, buffer, row = kind
        return remote(
            buffer.at[m], ends(side, 1, m)[1], relay_s.at[row, m], rs.at[side, m], lat=relay_end
        )

    def send_halo(kind, m):
        for side, sends, _, where, by_relay, relay in sides:
            @pl.when(jnp.logical_and(sends, jnp.logical_not(by_relay)))
            def _():
                direct(kind, side, 0, m, where).start()
                direct(kind, side, 1, m, where).start()

            @pl.when(by_relay)
            def _():
                to_relay(kind, side, m, relay).start()
                direct(kind, side, 0, m, where).start()

    def recv_halo(kind, m):
        for side, _, receives, where, _, _ in sides:
            @pl.when(receives)
            def _():
                direct(kind, side, None, m, where).wait_recv()

    def drain_halo(kind, m):
        for side, sends, _, where, _, _ in sides:
            @pl.when(sends)
            def _():
                direct(kind, side, None, m, where).wait_send()

        for side, relay in ((0, relay_up), (1, relay_down)):
            @pl.when(r == relay)
            def _():
                from_relay(kind, side, m).wait_send()

    def pass_on(kind, m):
        for side, relay in ((0, relay_up), (1, relay_down)):
            @pl.when(r == relay)
            def _():
                to_relay(kind, side, m, relay_end).wait_recv()
                from_relay(kind, side, m).start()

    for m in range(members):
        pltpu.make_async_copy(
            feat.at[m], feat_rows.at[pl.ds(1, 2), m, pl.ds(0, lon)], load_sem.at[m]
        ).wait()
        send_halo(feat_halo, m)

    feat_rows[:, :, lon:, :] = jnp.zeros((4, members, lon_pad - lon, LANE), BF16)
    shifted[:, lon:, :] = jnp.zeros((members, lon_pad - lon, shifted.shape[2]), BF16)

    @pl.when(r == 0)
    def _():
        for m in range(members):
            feat_rows[0, m, 0:lon] = jnp.zeros((lon, LANE), BF16)
            hgrad[0, m] = jnp.zeros((lon, LANE), BF16)
            grad_field[m, 0] = jnp.zeros((VP, lon_pad), BF16)
            for q in range(4):
                part_in[4 + q, m] = jnp.zeros((VP, third), BF16)

    @pl.when(r == LAT - 1)
    def _():
        for m in range(members):
            feat_rows[3, m, 0:lon] = jnp.zeros((lon, LANE), BF16)
            hgrad[3, m] = jnp.zeros((lon, LANE), BF16)
            grad_field[m, 3] = jnp.zeros((VP, lon_pad), BF16)
            for q in range(4):
                part_in[q, m] = jnp.zeros((VP, third), BF16)

    w_inner[...] = jnp.zeros(w_inner.shape, BF16)
    w_inner_back[...] = jnp.zeros(w_inner_back.shape, BF16)
    w_head[...] = jnp.zeros(w_head.shape, BF16)
    w_head_back[...] = jnp.zeros(w_head_back.shape, BF16)
    for a in range(3):
        for b in range(3):
            block = kin[a * 3 + b]
            block_t = transposed(block)
            head_t = ht[a * 3 + b]
            nv = head_t.shape[0]
            for o in range(2):
                cols = slice((o * 3 + b) * LANE, (o * 3 + b + 1) * LANE)
                w_inner[(o + a) * LANE:(o + a + 1) * LANE, cols] = block
                e = o - a + 2
                w_inner_back[e * LANE:(e + 1) * LANE, cols] = block_t
                row = o - a + 2
                w_head[row * VP:row * VP + nv, b * 2 * LANE + o * LANE:b * 2 * LANE + (o + 1) * LANE] = head_t
            w_head_back[(2 - a) * VP:(2 - a) * VP + nv, b * LANE:(b + 1) * LANE] = head_t

    def column(ref, fill):
        nv = ref.shape[1]
        row = jnp.concatenate([ref[...], jnp.full((1, LANE - nv), fill, F32)], axis=1)
        return jnp.transpose(jnp.broadcast_to(row, (LANE, LANE)))[0:VP]

    widths = column(width, 1.0)
    inverse = 1.0 / (widths * widths)
    scaling = jnp.sqrt(0.5 * math.log2(math.e) * inverse)
    factor = column(weight, 0.0) * inverse / scaling
    prm[0] = scaling
    prm[1] = factor * (2.0 / (MEM * members - 1))
    prm[2] = factor * 2.0
    target_buf[...] = jnp.zeros(target_buf.shape, F32)
    for quarter in range(4):
        for row in range(2):
            @pl.when(d == row * 4 + quarter)
            def _():
                stop = min((quarter + 1) * third, lon)
                target_buf[0:truth.shape[0], 0:stop - quarter * third] = truth[:, row, quarter * third:stop]

    def lanes(index):
        return slice(index * LANE, (index + 1) * LANE)

    def forward(m):
        recv_halo(feat_halo, m)
        rows = jnp.concatenate([feat_rows[e, m, 0:lon] for e in range(4)], axis=1)
        wide[...] = jnp.dot(rows, w_inner[...], preferred_element_type=F32)
        for o in range(2):
            pre = (
                roll_rows(wide[:, lanes(o * 3)], 1)
                + wide[:, lanes(o * 3 + 1)]
                + roll_rows(wide[:, lanes(o * 3 + 2)], -1)
            )
            square = pre * pre
            th = jnp.tanh(GELU_A * pre * (1.0 + GELU_B * square))
            cdf = 0.5 + 0.5 * th
            hidden = pre * cdf
            grad = cdf + 0.5 * pre * (1.0 - th * th) * (GELU_A * (1.0 + 3.0 * GELU_B * square))
            slope[m, :, lanes(o)] = grad.astype(BF16)
            shifted[m, 0:lon, lanes(o)] = roll_rows(hidden, 1).astype(BF16)
            shifted[m, 0:lon, lanes(2 + o)] = hidden.astype(BF16)
            shifted[m, 0:lon, lanes(4 + o)] = roll_rows(hidden, -1).astype(BF16)
        slot = m
        for q in range(4):
            sums = lax.dot_general(
                w_head[...], shifted[m, q * third:(q + 1) * third, :],
                (((1,), (1,)), ((), ())), preferred_element_type=F32,
            )
            part_out[q, m] = sums[0:VP].astype(BF16)
            own_field[slot, 0, :, q * third:(q + 1) * third] = sums[VP:2 * VP]
            own_field[slot, 1, :, q * third:(q + 1) * third] = sums[2 * VP:3 * VP]
            part_out[4 + q, m] = sums[3 * VP:4 * VP].astype(BF16)
        send_halo(part_halo, m)

    chunks = VP // 16

    def tile(t):
        return pl.ds(t * 16 if isinstance(t, int) else pl.multiple_of(t * 16, 16), 16)

    def field_copy(m, t, k):
        p = mem_peer(k)
        return remote(
            field_out.at[p, m, tile(t)], values_in.at[d, m, tile(t)],
            a2_s.at[t], a2_r.at[t], mem=p,
        )

    def finish_field(m):
        recv_halo(part_halo, m)
        slot = m
        for row in range(2):
            for q in range(4):
                total = own_field[slot, row, :, q * third:(q + 1) * third] + part_in[
                    (1 - row) * 4 + q, m
                ].astype(F32)
                field_out[row * 4 + q, m] = total.astype(BF16)
        for t in range(chunks):
            for k in range(1, MEM):
                field_copy(m, t, k).start()
        values_in[d, m] = field_out[d, m]

    pass_on(feat_halo, 0)
    pass_on(feat_halo, 1)

    def forward_step(m, carry):
        forward(m)

        @pl.when(m == 0)
        def _():
            for n in range(2, members):
                pass_on(feat_halo, n)

        @pl.when(m > 0)
        def _():
            pass_on(part_halo, m - 1)

        return carry

    def finish_step(m, carry):
        finish_field(m)
        return carry

    lax.fori_loop(0, members, forward_step, 0)
    pass_on(part_halo, members - 1)
    lax.fori_loop(0, members, finish_step, 0)

    grad_out = field_out
    count = MEM * members
    own_row = 1 + d // 4
    own_lane = lax.rem(d, 4) * third

    def place(j):
        return slice((j // 2) * 16, (j // 2 + 1) * 16), slice((j % 2) * third, (j % 2 + 1) * third)

    def back_copy(t, k):
        p = mem_peer(k)
        rows = tile(t)
        return remote(
            grad_out.at[p, :, rows],
            grad_field.at[:, own_row, rows, pl.ds(pl.multiple_of(own_lane, LANE), third)],
            b2_s.at[t], b2_r.at[t], mem=p,
        )

    block = 8
    lane_groups = third // LANE
    used_groups = -(-truth.shape[0] // 8)

    def pair_chunk(t, carry):
        rows16 = tile(t)

        others = pl.ds(0, MEM - 1)
        remote(
            field_out.at[others, :, rows16], values_in.at[others, :, rows16],
            a2_s.at[t], a2_r.at[t], mem=mem_peer(1),
        ).wait()
        scale = jnp.concatenate([prm[0, rows16]] * lane_groups, axis=1)
        for j in range(count):
            rows, cols = place(j)
            wide[rows, cols] = values_in[j // members, j % members, rows16].astype(F32) * scale

        def group(unit, inner):
            sub = unit // lane_groups
            lane = lax.rem(unit, lane_groups) * LANE

            def at(j):
                return (
                    pl.ds(pl.multiple_of((j // 2) * 16 + sub * 8, 8), 8),
                    pl.ds(pl.multiple_of((j % 2) * third + lane, LANE), LANE),
                )

            rows8 = pl.ds(pl.multiple_of(t * 16 + sub * 8, 8), 8)
            target = target_buf[rows8, pl.ds(pl.multiple_of(lane, LANE), LANE)] * prm[0, rows8]
            pair_weight = prm[1, rows8]
            truth_weight = prm[2, rows8]

            def term(x, y):
                u = x - y
                return u * jnp.exp2(u * (y - x))

            for i0 in range(0, count, block):
                xi = [wide[at(i0 + i)] for i in range(block)]
                sums = [None] * block
                for i in range(block):
                    for j in range(i + 1, block):
                        w = term(xi[j], xi[i])
                        sums[i] = w if sums[i] is None else sums[i] + w
                        sums[j] = -w if sums[j] is None else sums[j] - w
                if i0 > 0:
                    sums = [s + wide[at(count + i0 + i)] for i, s in enumerate(sums)]
                for j0 in range(i0 + block, count, 4):
                    xj = [wide[at(j0 + j)] for j in range(4)]
                    back = [None] * 4
                    for j in range(4):
                        for i in range(block):
                            w = term(xj[j], xi[i])
                            sums[i] = sums[i] + w
                            back[j] = -w if back[j] is None else back[j] - w
                    for j in range(4):
                        old = back[j] if i0 == 0 else wide[at(count + j0 + j)] + back[j]
                        wide[at(count + j0 + j)] = old
                for i in range(block):
                    near = term(xi[i], target)
                    wide[at(count + i0 + i)] = pair_weight * sums[i] + truth_weight * near
            return inner

        subs = jnp.minimum(2, used_groups - 2 * t)
        lax.fori_loop(0, subs * lane_groups, group, 0)
        keep = lax.broadcasted_iota(jnp.int32, (16, third), 0) < subs * 8
        for j in range(count):
            rows, cols = place(count + j)
            grad_out[j // members, j % members, rows16] = jnp.where(keep, wide[rows, cols], 0.0).astype(BF16)
        for k in range(1, MEM):
            back_copy(t, k).start()
        grad_field[:, own_row, rows16, pl.ds(pl.multiple_of(own_lane, LANE), third)] = grad_out[d, :, rows16]
        return carry

    lax.fori_loop(0, chunks, pair_chunk, 0)

    def wait_back(t, carry):
        others = pl.ds(0, MEM - 1)
        remote(
            grad_out.at[others, :, tile(t)], values_in.at[others, :, tile(t)],
            b2_s.at[t], b2_r.at[t], mem=mem_peer(1),
        ).wait()
        send_halo(gfield_halo, t)

        @pl.when(t > 0)
        def _():
            pass_on(gfield_halo, t - 1)

        return carry

    lax.fori_loop(0, chunks, wait_back, 0)

    inner_acc[...] = jnp.zeros(inner_acc.shape, F32)
    head_acc[...] = jnp.zeros(head_acc.shape, F32)

    def at_rows(start, size):
        return pl.ds(pl.multiple_of(start, 8), size)

    def device_sum(src, dst, r1, r2, r3, sb, db, sems):
        half_rows = src.shape[0] // 2
        piece_rows = half_rows // MEM
        my_half = half * half_rows
        my_piece = my_half + d * piece_rows

        def scatter_pair():
            return remote(
                src.at[at_rows((1 - half) * half_rows, half_rows)], r1, sems.at[0], sems.at[1], lat=partner
            )

        def scatter(k):
            return remote(
                sb.at[mem_peer(k)], r2.at[k], sems.at[2], sems.at[3], mem=mem_peer(k),
            )

        def share(k):
            return remote(r3.at[seat], r3.at[seat], sems.at[4], sems.at[5], lat=lat_peer(k))

        def gather(k):
            piece = db.at[half, d]
            return remote(piece, piece, sems.at[6], sems.at[7], mem=mem_peer(k))

        def gather_pair():
            piece = db.at[half]
            return remote(piece, piece, sems.at[8], sems.at[9], lat=partner)

        def each(copy_of, act):
            for k in range(1, MEM):
                act(copy_of(k))

        start = lambda c: c.start()

        def wait_all(n, buffer, where):
            slabs = buffer.at[pl.ds(0, MEM - 1)]
            remote(slabs, slabs, sems.at[2 * n], sems.at[2 * n + 1], **where).wait()

        def step_0():
            scatter_pair().start()

        def step_1():
            scatter_pair().wait()
            mine = at_rows(my_half, half_rows)
            src[mine] = src[mine] + r1[...]
            for p in range(MEM):
                sb[p] = src[at_rows(my_half + p * piece_rows, piece_rows)].astype(BF16)
            each(scatter, start)

        def step_2():
            wait_all(1, r2, {"mem": mem_peer(1)})
            mine = at_rows(my_piece, piece_rows)
            total = src[mine]
            for k in range(1, MEM):
                total = total + r2[k].astype(F32)
            r3[seat] = total.astype(BF16)
            each(share, start)

        def step_3():
            wait_all(2, r3, {"lat": lat_peer(1)})
            total = r3[0].astype(F32)
            for k in range(1, MEM):
                total = total + r3[k].astype(F32)
            db[half, d] = (total * (1.0 / (2 * LAT * lon))).astype(BF16)
            each(gather, start)

        def step_4():
            wait_all(3, db.at[0], {"mem": mem_peer(1)})
            gather_pair().start()

        def step_5():
            gather_pair().wait()
            for h in range(2):
                for p in range(MEM):
                    start_row = h * half_rows + p * piece_rows
                    dst[start_row:start_row + piece_rows] = db[h, p].astype(F32)

        return step_0, step_1, step_2, step_3, step_4, step_5

    head_steps = device_sum(hs_in, hs_out, hs_r1, hs_r2, hs_r3, hs_sb, hs_db, hsum_sems)
    inner_steps = device_sum(is_in, is_out, is_r1, is_r2, is_r3, is_sb, is_db, isum_sems)

    def head_gradient(m, carry):
        fields = grad_field[m].reshape(4 * VP, lon_pad)
        head_acc[...] += jnp.dot(fields, shifted[m], preferred_element_type=F32)
        return carry

    def halo_tiles(t, carry):
        recv_halo(gfield_halo, t)
        return carry

    pass_on(gfield_halo, chunks - 1)
    lax.fori_loop(0, chunks, halo_tiles, 0)
    lax.fori_loop(0, members, head_gradient, 0)
    for a in range(3):
        for b in range(3):
            base = (a * 3 + b) * VP
            hs_in[base:base + VP] = (
                head_acc[(2 - a) * VP:(3 - a) * VP, lanes(b * 2)]
                + head_acc[(3 - a) * VP:(4 - a) * VP, lanes(b * 2 + 1)]
            )
    hs_in[9 * VP:] = jnp.zeros((hs_in.shape[0] - 9 * VP, LANE), F32)
    head_steps[0]()

    def backward(m, carry):
        for i in range(2):
            stack = [grad_field[m, i + j] for j in range(3)]
            stack.append(jnp.zeros((2 * LANE - 3 * VP, lon_pad), BF16))
            columns = transposed(jnp.concatenate(stack, axis=0))
            wide[:, 0:3 * LANE] = jnp.dot(
                columns[0:lon], w_head_back[...], preferred_element_type=F32
            )
            total = (
                roll_rows(wide[:, lanes(0)], -1) + wide[:, lanes(1)] + roll_rows(wide[:, lanes(2)], 1)
            )
            hg = total * slope[m, :, lanes(i)].astype(F32)
            hgrad[1 + i, m] = hg.astype(BF16)
            tail = jnp.zeros((lon_pad - lon, LANE), F32)
            for b in range(3):
                moved = hg if b == 1 else roll_rows(hg, b - 1)
                hgrad_t[(i * 3 + b) * LANE:(i * 3 + b + 1) * LANE, :] = jnp.transpose(
                    jnp.concatenate([moved, tail], axis=0)
                ).astype(BF16)
        send_halo(hgrad_halo, m)
        rows = jnp.concatenate([feat_rows[e, m] for e in range(4)], axis=1)
        inner_acc[...] += jnp.dot(hgrad_t[...], rows, preferred_element_type=F32)
        @pl.when(m >= 2)
        def _():
            pass_on(hgrad_halo, m - 2)

        for n in (1, 2):
            @pl.when(m == 2 * n - 1)
            def _():
                head_steps[n]()

        return carry

    lax.fori_loop(0, members, backward, 0)
    for a in range(3):
        for b in range(3):
            ab = a * 3 + b
            is_in[ab * LANE:(ab + 1) * LANE] = jnp.transpose(
                inner_acc[b * LANE:(b + 1) * LANE, lanes(a)]
                + inner_acc[(3 + b) * LANE:(4 + b) * LANE, lanes(1 + a)]
            )

    def gf_copy(m):
        return pltpu.make_async_copy(gf_buf.at[lax.rem(m, 2)], gf_out.at[m], out_sem.at[lax.rem(m, 2)])

    inner_steps[0]()

    def last(m, carry):
        recv_halo(hgrad_halo, m)

        @pl.when(m >= 2)
        def _():
            gf_copy(m - 2).wait()

        rows = jnp.concatenate([hgrad[e, m] for e in range(4)], axis=1)
        wide[...] = jnp.dot(rows, w_inner_back[...], preferred_element_type=F32)
        for o in range(2):
            total = (
                roll_rows(wide[:, lanes(o * 3)], -1)
                + wide[:, lanes(o * 3 + 1)]
                + roll_rows(wide[:, lanes(o * 3 + 2)], 1)
            )
            gf_buf[lax.rem(m, 2), o] = total.astype(BF16)
        gf_copy(m).start()

        for n in range(members):
            @pl.when(m == n)
            def _():
                inner_steps[n + 1]()
                if n > 0:
                    head_steps[n + 2]()
                if n == 0:
                    pass_on(hgrad_halo, members - 2)
                    pass_on(hgrad_halo, members - 1)

        return carry

    lax.fori_loop(0, members, last, 0)

    for m in range(members):
        drain_halo(feat_halo, m)
        drain_halo(part_halo, m)
        drain_halo(hgrad_halo, m)
    for t in range(chunks):
        drain_halo(gfield_halo, t)
    for m in range(max(members - 2, 0), members):
        gf_copy(m).wait()
    for ab in range(9):
        gh_out[ab] = hs_out[ab * VP:ab * VP + gh_out.shape[1]]
    inner_steps[5]()
    for ab in range(9):
        gi_out[ab] = is_out[ab * LANE:(ab + 1) * LANE]


def sum_scratch(rows):
    piece = rows // 2 // MEM
    return [
        pltpu.VMEM((rows, LANE), F32),
        pltpu.VMEM((rows, LANE), F32),
        pltpu.VMEM((rows // 2, LANE), F32),
        pltpu.VMEM((MEM, piece, LANE), BF16),
        pltpu.VMEM((MEM, piece, LANE), BF16),
        pltpu.VMEM((MEM, piece, LANE), BF16),
        pltpu.VMEM((2, MEM, piece, LANE), BF16),
    ]


def shards(features, conv_inner, conv_head, truth, kernel_width, var_weight):
    members, band, lon, channels = features.shape
    variables = conv_head.shape[3]
    lon_pad = -(-lon // (4 * LANE)) * 4 * LANE
    third = lon_pad // 4
    kin = conv_inner.reshape(9, channels, channels)
    ht = jnp.swapaxes(conv_head.reshape(9, channels, variables), 1, 2)
    width = kernel_width.reshape(1, variables)
    weight = var_weight.reshape(1, variables)

    any_spec = pl.BlockSpec(memory_space=pl.ANY)
    vmem = pl.BlockSpec(memory_space=pltpu.VMEM)
    dma = pltpu.SemaphoreType.DMA
    scratch = [
        pltpu.VMEM((4, members, lon_pad, LANE), BF16),
        pltpu.VMEM((lon, 6 * LANE), F32),
        pltpu.VMEM((members, lon_pad, 6 * LANE), BF16),
        pltpu.VMEM((members, lon, 2 * LANE), BF16),
        pltpu.VMEM((4, members, lon, LANE), BF16),
        pltpu.VMEM((6 * LANE, lon_pad), BF16),
        pltpu.VMEM((members, 2, VP, lon_pad), F32),
        pltpu.VMEM((MEM, members, VP, third), BF16),
        pltpu.VMEM((MEM, members, VP, third), BF16),
        pltpu.VMEM((MEM, members, VP, third), BF16),
        pltpu.VMEM((MEM, members, VP, third), BF16),
        pltpu.VMEM((members, 4, VP, lon_pad), BF16),
        pltpu.VMEM((4 * LANE, 6 * LANE), BF16),
        pltpu.VMEM((4 * VP, 6 * LANE), BF16),
        pltpu.VMEM((2 * LANE, 3 * LANE), BF16),
        pltpu.VMEM((4 * LANE, 6 * LANE), BF16),
        pltpu.VMEM((members, lon // 2, LANE), BF16),
        pltpu.VMEM((members, 2, VP, third), BF16),
        pltpu.VMEM((VP // 16, members // 2, 16, lon_pad), BF16),
        pltpu.VMEM((members, lon // 2, LANE), BF16),
        pltpu.VMEM((6 * LANE, 4 * LANE), F32),
        pltpu.VMEM((4 * VP, 6 * LANE), F32),
        pltpu.VMEM((2, 2, lon, LANE), BF16),
        pltpu.VMEM((3, VP, LANE), F32),
        pltpu.VMEM((VP, third), F32),
        *sum_scratch(HEAD_ROWS),
        *sum_scratch(9 * LANE),
        dma((members,)),
        dma((2, members)), dma((2, members)),
        dma((2, members)), dma((2, members)),
        dma((VP // 16,)), dma((VP // 16,)),
        dma((VP // 16,)), dma((VP // 16,)),
        dma((2, VP // 16)), dma((2, VP // 16)),
        dma((2, members)), dma((2, members)),
        dma((10,)), dma((10,)),
        dma((2,)),
        dma((4, VP // 16)), dma((4, VP // 16)),
    ]
    grad_features, inner, head = pl.pallas_call(
        whole_block,
        out_shape=(
            jax.ShapeDtypeStruct(features.shape, BF16),
            jax.ShapeDtypeStruct((9, channels, channels), F32),
            jax.ShapeDtypeStruct((9, variables, channels), F32),
        ),
        in_specs=[any_spec, vmem, vmem, vmem, vmem, vmem],
        out_specs=(any_spec, vmem, vmem),
        scratch_shapes=scratch,
        compiler_params=pltpu.CompilerParams(
            collective_id=0, has_side_effects=True, vmem_limit_bytes=67043328
        ),
    )(features, kin, ht, width, weight, truth)
    return (
        grad_features,
        inner.reshape(3, 3, channels, channels),
        jnp.swapaxes(head, 1, 2).reshape(3, 3, channels, variables),
    )


def solution(mesh):
    in_specs = (P("mem", "lat", None, None), P(), P(), P(None, "lat", None), P(), P())
    out_specs = (P("mem", "lat", None, None), P(), P())
    return jax.shard_map(shards, mesh=mesh, in_specs=in_specs, out_specs=out_specs, check_vma=False)
```

```python
import math
import jax
import jax.numpy as jnp
from jax import lax
from jax.experimental import pallas as pl
from jax.experimental.pallas import tpu as pltpu
from jax.sharding import PartitionSpec as P

MESH_ID = pl.DeviceIdType.MESH
F32 = jnp.float32
BF16 = jnp.bfloat16
LANE = 128
VP = 80
MEM = 8
LAT = 16
HEAD_ROWS = 768
RELAYS = (0, LAT - 1)
GELU_A = math.sqrt(2.0 / math.pi)
GELU_B = 0.044715


def roll_rows(values, shift):
    return pltpu.roll(values, shift % values.shape[0], 0)


def transposed(values):
    return jnp.transpose(values.astype(F32)).astype(BF16)


def whole_block(
    feat, kin, ht, width, weight, truth,
    gf_out, gi_out, gh_out,
    feat_rows, wide, shifted, slope, hgrad, hgrad_t, own_field,
    part_out, part_in, field_out, values_in, grad_field,
    w_inner, w_head, w_head_back, w_inner_back,
    feat_relay, part_relay, gfield_relay, hgrad_relay,
    inner_acc, head_acc, gf_buf, prm, target_buf,
    hs_in, hs_out, hs_r1, hs_r2, hs_r3, hs_sb, hs_db,
    is_in, is_out, is_r1, is_r2, is_r3, is_sb, is_db,
    load_sem, fh_s, fh_r, ph_s, ph_r, a2_s, a2_r, b2_s, b2_r, gh_s, gh_r, hh_s, hh_r,
    hsum_sems, isum_sems, out_sem, relay_s, relay_r,
):
    lon = feat.shape[2]
    lon_pad = grad_field.shape[3]
    members = feat.shape[0]
    third = lon_pad // 4
    d = lax.axis_index("mem")
    r = lax.axis_index("lat")
    has_up = r > 0
    has_down = r < LAT - 1
    above = lax.rem(r + LAT - 1, LAT)
    below = lax.rem(r + 1, LAT)
    half = lax.rem(r, 2)
    seat = r // 2

    def mem_peer(k):
        return lax.rem(d + k, MEM)

    def lat_peer(k):
        return lax.rem(seat + k, MEM) * 2 + half

    partner = r + 1 - 2 * half

    def remote(src, dst, ss, rs, **where):
        return pltpu.make_async_remote_copy(
            src_ref=src, dst_ref=dst, send_sem=ss, recv_sem=rs,
            device_id=where, device_id_type=MESH_ID,
        )

    barrier = pltpu.get_barrier_semaphore()
    for k in range(1, MEM):
        pl.semaphore_signal(barrier, inc=1, device_id={"mem": mem_peer(k)}, device_id_type=MESH_ID)
    for k in range(1, LAT):
        pl.semaphore_signal(
            barrier, inc=1, device_id={"lat": lax.rem(r + k, LAT)}, device_id_type=MESH_ID
        )

    def load(m, row):
        return pltpu.make_async_copy(
            feat.at[m, row], feat_rows.at[1 + row, m, pl.ds(0, lon)], load_sem.at[m]
        )

    for m in range(members):
        for row in range(2):
            load(m, row).start()

    pl.semaphore_wait(barrier, MEM - 1 + LAT - 1)

    mid_up = r == LAT // 2 - 1
    mid_down = r == LAT // 2
    relay_down = RELAYS[0]
    relay_up = RELAYS[1]
    is_relay = jnp.logical_or(r == relay_down, r == relay_up)
    relay_end = jnp.where(r == relay_down, LAT // 2, LAT // 2 - 1)
    part_rows = lon // 2

    def halo_rows(part):
        return pl.ds(0, lon) if part is None else pl.ds(part * part_rows, part_rows)

    def feat_ends(side, part, m):
        own, other = (1, 3) if side == 0 else (2, 0)
        return feat_rows.at[own, m, halo_rows(part)], feat_rows.at[other, m, halo_rows(part)]

    def part_ends(side, part, m):
        slots = pl.ds(side * 4, 4) if part is None else pl.ds(side * 4 + part * 2, 2)
        return part_out.at[slots, m], part_in.at[slots, m]

    def gfield_ends(side, part, t):
        own, other = (1, 3) if side == 0 else (2, 0)
        rows = pl.ds(pl.multiple_of(t * 16, 16), 16)
        which = pl.ds(0, members) if part is None else pl.ds(part * (members // 2), members // 2)
        return grad_field.at[which, own, rows], grad_field.at[which, other, rows]

    def hgrad_ends(side, part, m):
        own, other = (1, 3) if side == 0 else (2, 0)
        return hgrad.at[own, m, halo_rows(part)], hgrad.at[other, m, halo_rows(part)]

    feat_halo = (feat_ends, fh_s, fh_r, feat_relay, 0)
    part_halo = (part_ends, ph_s, ph_r, part_relay, 1)
    gfield_halo = (gfield_ends, gh_s, gh_r, gfield_relay, 2)
    hgrad_halo = (hgrad_ends, hh_s, hh_r, hgrad_relay, 3)

    sides = (
        (0, has_up, has_down, above, mid_down, relay_up),
        (1, has_down, has_up, below, mid_up, relay_down),
    )

    def direct(kind, side, part, m, where):
        ends, ss, rs, _, _ = kind
        src, dst = ends(side, part, m)
        return remote(src, dst, ss.at[side, m], rs.at[side, m], lat=where)

    def to_relay(kind, side, m, where):
        ends, ss, _, buffer, row = kind
        return remote(ends(side, 1, m)[0], buffer.at[m], ss.at[side, m], relay_r.at[row, m], lat=where)

    def from_relay(kind, side, m):
        ends, _, rs, buffer, row = kind
        return remote(
            buffer.at[m], ends(side, 1, m)[1], relay_s.at[row, m], rs.at[side, m], lat=relay_end
        )

    def send_halo(kind, m):
        for side, sends, _, where, by_relay, relay in sides:
            @pl.when(jnp.logical_and(sends, jnp.logical_not(by_relay)))
            def _():
                direct(kind, side, 0, m, where).start()
                direct(kind, side, 1, m, where).start()

            @pl.when(by_relay)
            def _():
                to_relay(kind, side, m, relay).start()
                direct(kind, side, 0, m, where).start()

    def recv_halo(kind, m):
        for side, _, receives, where, _, _ in sides:
            @pl.when(receives)
            def _():
                direct(kind, side, None, m, where).wait_recv()

    def drain_halo(kind, m):
        for side, sends, _, where, _, _ in sides:
            @pl.when(sends)
            def _():
                direct(kind, side, None, m, where).wait_send()

        for side, relay in ((0, relay_up), (1, relay_down)):
            @pl.when(r == relay)
            def _():
                from_relay(kind, side, m).wait_send()

    def pass_on(kind, m):
        for side, relay in ((0, relay_up), (1, relay_down)):
            @pl.when(r == relay)
            def _():
                to_relay(kind, side, m, relay_end).wait_recv()
                from_relay(kind, side, m).start()

    for m in range(members):
        pltpu.make_async_copy(
            feat.at[m], feat_rows.at[pl.ds(1, 2), m, pl.ds(0, lon)], load_sem.at[m]
        ).wait()
        send_halo(feat_halo, m)

    feat_rows[:, :, lon:, :] = jnp.zeros((4, members, lon_pad - lon, LANE), BF16)
    shifted[:, lon:, :] = jnp.zeros((members, lon_pad - lon, shifted.shape[2]), BF16)

    @pl.when(r == 0)
    def _():
        for m in range(members):
            feat_rows[0, m, 0:lon] = jnp.zeros((lon, LANE), BF16)
            hgrad[0, m] = jnp.zeros((lon, LANE), BF16)
            grad_field[m, 0] = jnp.zeros((VP, lon_pad), BF16)
            for q in range(4):
                part_in[4 + q, m] = jnp.zeros((VP, third), BF16)

    @pl.when(r == LAT - 1)
    def _():
        for m in range(members):
            feat_rows[3, m, 0:lon] = jnp.zeros((lon, LANE), BF16)
            hgrad[3, m] = jnp.zeros((lon, LANE), BF16)
            grad_field[m, 3] = jnp.zeros((VP, lon_pad), BF16)
            for q in range(4):
                part_in[q, m] = jnp.zeros((VP, third), BF16)

    w_inner[...] = jnp.zeros(w_inner.shape, BF16)
    w_inner_back[...] = jnp.zeros(w_inner_back.shape, BF16)
    w_head[...] = jnp.zeros(w_head.shape, BF16)
    w_head_back[...] = jnp.zeros(w_head_back.shape, BF16)
    for a in range(3):
        for b in range(3):
            block = kin[a * 3 + b]
            block_t = transposed(block)
            head_t = ht[a * 3 + b]
            nv = head_t.shape[0]
            for o in range(2):
                cols = slice((o * 3 + b) * LANE, (o * 3 + b + 1) * LANE)
                w_inner[(o + a) * LANE:(o + a + 1) * LANE, cols] = block
                e = o - a + 2
                w_inner_back[e * LANE:(e + 1) * LANE, cols] = block_t
                row = o - a + 2
                w_head[row * VP:row * VP + nv, b * 2 * LANE + o * LANE:b * 2 * LANE + (o + 1) * LANE] = head_t
            w_head_back[(2 - a) * VP:(2 - a) * VP + nv, b * LANE:(b + 1) * LANE] = head_t

    def column(ref, fill):
        nv = ref.shape[1]
        row = jnp.concatenate([ref[...], jnp.full((1, LANE - nv), fill, F32)], axis=1)
        return jnp.transpose(jnp.broadcast_to(row, (LANE, LANE)))[0:VP]

    widths = column(width, 1.0)
    inverse = 1.0 / (widths * widths)
    scaling = jnp.sqrt(0.5 * math.log2(math.e) * inverse)
    factor = column(weight, 0.0) * inverse / scaling
    prm[0] = scaling
    prm[1] = factor * (2.0 / (MEM * members - 1))
    prm[2] = factor * 2.0
    target_buf[...] = jnp.zeros(target_buf.shape, F32)
    for quarter in range(4):
        for row in range(2):
            @pl.when(d == row * 4 + quarter)
            def _():
                stop = min((quarter + 1) * third, lon)
                target_buf[0:truth.shape[0], 0:stop - quarter * third] = truth[:, row, quarter * third:stop]

    def lanes(index):
        return slice(index * LANE, (index + 1) * LANE)

    def forward(m):
        recv_halo(feat_halo, m)
        rows = jnp.concatenate([feat_rows[e, m, 0:lon] for e in range(4)], axis=1)
        wide[...] = jnp.dot(rows, w_inner[...], preferred_element_type=F32)
        for o in range(2):
            pre = (
                roll_rows(wide[:, lanes(o * 3)], 1)
                + wide[:, lanes(o * 3 + 1)]
                + roll_rows(wide[:, lanes(o * 3 + 2)], -1)
            )
            square = pre * pre
            th = jnp.tanh(GELU_A * pre * (1.0 + GELU_B * square))
            cdf = 0.5 + 0.5 * th
            hidden = pre * cdf
            grad = cdf + 0.5 * pre * (1.0 - th * th) * (GELU_A * (1.0 + 3.0 * GELU_B * square))
            slope[m, :, lanes(o)] = grad.astype(BF16)
            shifted[m, 0:lon, lanes(o)] = roll_rows(hidden, 1).astype(BF16)
            shifted[m, 0:lon, lanes(2 + o)] = hidden.astype(BF16)
            shifted[m, 0:lon, lanes(4 + o)] = roll_rows(hidden, -1).astype(BF16)
        slot = m
        for q in range(4):
            sums = lax.dot_general(
                w_head[...], shifted[m, q * third:(q + 1) * third, :],
                (((1,), (1,)), ((), ())), preferred_element_type=F32,
            )
            part_out[q, m] = sums[0:VP].astype(BF16)
            own_field[slot, 0, :, q * third:(q + 1) * third] = sums[VP:2 * VP]
            own_field[slot, 1, :, q * third:(q + 1) * third] = sums[2 * VP:3 * VP]
            part_out[4 + q, m] = sums[3 * VP:4 * VP].astype(BF16)
        send_halo(part_halo, m)

    chunks = VP // 16

    def tile(t):
        return pl.ds(t * 16 if isinstance(t, int) else pl.multiple_of(t * 16, 16), 16)

    def field_copy(m, t, k):
        p = mem_peer(k)
        return remote(
            field_out.at[p, m, tile(t)], values_in.at[d, m, tile(t)],
            a2_s.at[t], a2_r.at[t], mem=p,
        )

    def finish_field(m):
        recv_halo(part_halo, m)
        slot = m
        for row in range(2):
            for q in range(4):
                total = own_field[slot, row, :, q * third:(q + 1) * third] + part_in[
                    (1 - row) * 4 + q, m
                ].astype(F32)
                field_out[row * 4 + q, m] = total.astype(BF16)
        early = members // 2

        @pl.when(m < early)
        def _():
            for t in range(chunks):
                for k in range(1, MEM):
                    field_copy(m, t, k).start()

        @pl.when(m == members - 1)
        def _():
            for t in range(chunks):
                for late in range(early, members):
                    for k in range(1, MEM):
                        field_copy(late, t, k).start()

        values_in[d, m] = field_out[d, m]

    pass_on(feat_halo, 0)
    pass_on(feat_halo, 1)

    def forward_step(m, carry):
        forward(m)

        @pl.when(m == 0)
        def _():
            for n in range(2, members):
                pass_on(feat_halo, n)

        @pl.when(m > 0)
        def _():
            pass_on(part_halo, m - 1)

        return carry

    def finish_step(m, carry):
        finish_field(m)
        return carry

    lax.fori_loop(0, members, forward_step, 0)
    pass_on(part_halo, members - 1)
    lax.fori_loop(0, members, finish_step, 0)

    grad_out = field_out
    count = MEM * members
    own_row = 1 + d // 4
    own_lane = lax.rem(d, 4) * third

    def place(j):
        return slice((j // 2) * 16, (j // 2 + 1) * 16), slice((j % 2) * third, (j % 2 + 1) * third)

    def back_copy(t, k):
        p = mem_peer(k)
        rows = tile(t)
        return remote(
            grad_out.at[p, :, rows],
            grad_field.at[:, own_row, rows, pl.ds(pl.multiple_of(own_lane, LANE), third)],
            b2_s.at[t], b2_r.at[t], mem=p,
        )

    block = 8
    lane_groups = third // LANE
    used_groups = -(-truth.shape[0] // 8)

    def pair_chunk(t, carry):
        rows16 = tile(t)

        others = pl.ds(0, MEM - 1)
        remote(
            field_out.at[others, :, rows16], values_in.at[others, :, rows16],
            a2_s.at[t], a2_r.at[t], mem=mem_peer(1),
        ).wait()
        scale = jnp.concatenate([prm[0, rows16]] * lane_groups, axis=1)
        for j in range(count):
            rows, cols = place(j)
            wide[rows, cols] = values_in[j // members, j % members, rows16].astype(F32) * scale

        def group(unit, inner):
            sub = unit // lane_groups
            lane = lax.rem(unit, lane_groups) * LANE

            def at(j):
                return (
                    pl.ds(pl.multiple_of((j // 2) * 16 + sub * 8, 8), 8),
                    pl.ds(pl.multiple_of((j % 2) * third + lane, LANE), LANE),
                )

            rows8 = pl.ds(pl.multiple_of(t * 16 + sub * 8, 8), 8)
            target = target_buf[rows8, pl.ds(pl.multiple_of(lane, LANE), LANE)] * prm[0, rows8]
            pair_weight = prm[1, rows8]
            truth_weight = prm[2, rows8]

            def term(x, y):
                u = x - y
                return u * jnp.exp2(u * (y - x))

            for i0 in range(0, count, block):
                xi = [wide[at(i0 + i)] for i in range(block)]
                sums = [None] * block
                for i in range(block):
                    for j in range(i + 1, block):
                        w = term(xi[j], xi[i])
                        sums[i] = w if sums[i] is None else sums[i] + w
                        sums[j] = -w if sums[j] is None else sums[j] - w
                if i0 > 0:
                    sums = [s + wide[at(count + i0 + i)] for i, s in enumerate(sums)]
                for j0 in range(i0 + block, count, 4):
                    xj = [wide[at(j0 + j)] for j in range(4)]
                    back = [None] * 4
                    for j in range(4):
                        for i in range(block):
                            w = term(xj[j], xi[i])
                            sums[i] = sums[i] + w
                            back[j] = -w if back[j] is None else back[j] - w
                    for j in range(4):
                        old = back[j] if i0 == 0 else wide[at(count + j0 + j)] + back[j]
                        wide[at(count + j0 + j)] = old
                for i in range(block):
                    near = term(xi[i], target)
                    wide[at(count + i0 + i)] = pair_weight * sums[i] + truth_weight * near
            return inner

        subs = jnp.minimum(2, used_groups - 2 * t)
        lax.fori_loop(0, subs * lane_groups, group, 0)
        keep = lax.broadcasted_iota(jnp.int32, (16, third), 0) < subs * 8
        for j in range(count):
            rows, cols = place(count + j)
            grad_out[j // members, j % members, rows16] = jnp.where(keep, wide[rows, cols], 0.0).astype(BF16)
        for k in range(1, MEM):
            back_copy(t, k).start()
        grad_field[:, own_row, rows16, pl.ds(pl.multiple_of(own_lane, LANE), third)] = grad_out[d, :, rows16]
        return carry

    lax.fori_loop(0, chunks, pair_chunk, 0)

    def wait_back(t, carry):
        pass_on(gfield_halo, t)
        others = pl.ds(0, MEM - 1)
        remote(
            grad_out.at[others, :, tile(t)], values_in.at[others, :, tile(t)],
            b2_s.at[t], b2_r.at[t], mem=mem_peer(1),
        ).wait()
        send_halo(gfield_halo, t)
        return carry

    lax.fori_loop(0, chunks, wait_back, 0)

    inner_acc[...] = jnp.zeros(inner_acc.shape, F32)
    head_acc[...] = jnp.zeros(head_acc.shape, F32)

    def at_rows(start, size):
        return pl.ds(pl.multiple_of(start, 8), size)

    def device_sum(src, dst, r1, r2, r3, sb, db, sems):
        half_rows = src.shape[0] // 2
        piece_rows = half_rows // MEM
        my_half = half * half_rows
        my_piece = my_half + d * piece_rows

        def scatter_pair():
            return remote(
                src.at[at_rows((1 - half) * half_rows, half_rows)], r1, sems.at[0], sems.at[1], lat=partner
            )

        def scatter(k):
            return remote(
                sb.at[mem_peer(k)], r2.at[k], sems.at[2], sems.at[3], mem=mem_peer(k),
            )

        def share(k):
            return remote(r3.at[seat], r3.at[seat], sems.at[4], sems.at[5], lat=lat_peer(k))

        def gather(k):
            piece = db.at[half, d]
            return remote(piece, piece, sems.at[6], sems.at[7], mem=mem_peer(k))

        def gather_pair():
            piece = db.at[half]
            return remote(piece, piece, sems.at[8], sems.at[9], lat=partner)

        def each(copy_of, act):
            for k in range(1, MEM):
                act(copy_of(k))

        start = lambda c: c.start()

        def wait_all(n, buffer, where):
            slabs = buffer.at[pl.ds(0, MEM - 1)]
            remote(slabs, slabs, sems.at[2 * n], sems.at[2 * n + 1], **where).wait()

        def step_0():
            scatter_pair().start()

        def step_1():
            scatter_pair().wait()
            mine = at_rows(my_half, half_rows)
            src[mine] = src[mine] + r1[...]
            for p in range(MEM):
                sb[p] = src[at_rows(my_half + p * piece_rows, piece_rows)].astype(BF16)
            each(scatter, start)

        def step_2():
            wait_all(1, r2, {"mem": mem_peer(1)})
            mine = at_rows(my_piece, piece_rows)
            total = src[mine]
            for k in range(1, MEM):
                total = total + r2[k].astype(F32)
            r3[seat] = total.astype(BF16)
            each(share, start)

        def step_3():
            wait_all(2, r3, {"lat": lat_peer(1)})
            total = r3[0].astype(F32)
            for k in range(1, MEM):
                total = total + r3[k].astype(F32)
            db[half, d] = (total * (1.0 / (2 * LAT * lon))).astype(BF16)
            each(gather, start)

        def step_4():
            wait_all(3, db.at[0], {"mem": mem_peer(1)})
            gather_pair().start()

        def step_5():
            gather_pair().wait()
            for h in range(2):
                for p in range(MEM):
                    start_row = h * half_rows + p * piece_rows
                    dst[start_row:start_row + piece_rows] = db[h, p].astype(F32)

        return step_0, step_1, step_2, step_3, step_4, step_5

    head_steps = device_sum(hs_in, hs_out, hs_r1, hs_r2, hs_r3, hs_sb, hs_db, hsum_sems)
    inner_steps = device_sum(is_in, is_out, is_r1, is_r2, is_r3, is_sb, is_db, isum_sems)

    def head_gradient(m, carry):
        fields = grad_field[m].reshape(4 * VP, lon_pad)
        head_acc[...] += jnp.dot(fields, shifted[m], preferred_element_type=F32)
        return carry

    def halo_tiles(t, carry):
        recv_halo(gfield_halo, t)
        return carry

    lax.fori_loop(0, chunks, halo_tiles, 0)
    lax.fori_loop(0, members, head_gradient, 0)
    for a in range(3):
        for b in range(3):
            base = (a * 3 + b) * VP
            hs_in[base:base + VP] = (
                head_acc[(2 - a) * VP:(3 - a) * VP, lanes(b * 2)]
                + head_acc[(3 - a) * VP:(4 - a) * VP, lanes(b * 2 + 1)]
            )
    hs_in[9 * VP:] = jnp.zeros((hs_in.shape[0] - 9 * VP, LANE), F32)
    head_steps[0]()

    def backward(m, carry):
        for i in range(2):
            stack = [grad_field[m, i + j] for j in range(3)]
            stack.append(jnp.zeros((2 * LANE - 3 * VP, lon_pad), BF16))
            columns = transposed(jnp.concatenate(stack, axis=0))
            wide[:, 0:3 * LANE] = jnp.dot(
                columns[0:lon], w_head_back[...], preferred_element_type=F32
            )
            total = (
                roll_rows(wide[:, lanes(0)], -1) + wide[:, lanes(1)] + roll_rows(wide[:, lanes(2)], 1)
            )
            hg = total * slope[m, :, lanes(i)].astype(F32)
            hgrad[1 + i, m] = hg.astype(BF16)
            tail = jnp.zeros((lon_pad - lon, LANE), F32)
            for b in range(3):
                moved = hg if b == 1 else roll_rows(hg, b - 1)
                hgrad_t[(i * 3 + b) * LANE:(i * 3 + b + 1) * LANE, :] = jnp.transpose(
                    jnp.concatenate([moved, tail], axis=0)
                ).astype(BF16)
        send_halo(hgrad_halo, m)
        rows = jnp.concatenate([feat_rows[e, m] for e in range(4)], axis=1)
        inner_acc[...] += jnp.dot(hgrad_t[...], rows, preferred_element_type=F32)
        @pl.when(m >= 2)
        def _():
            pass_on(hgrad_halo, m - 2)

        for n in (1, 2):
            @pl.when(m == 2 * n - 1)
            def _():
                head_steps[n]()

        return carry

    lax.fori_loop(0, members, backward, 0)
    for a in range(3):
        for b in range(3):
            ab = a * 3 + b
            is_in[ab * LANE:(ab + 1) * LANE] = jnp.transpose(
                inner_acc[b * LANE:(b + 1) * LANE, lanes(a)]
                + inner_acc[(3 + b) * LANE:(4 + b) * LANE, lanes(1 + a)]
            )

    def gf_copy(m):
        return pltpu.make_async_copy(gf_buf.at[lax.rem(m, 2)], gf_out.at[m], out_sem.at[lax.rem(m, 2)])

    inner_steps[0]()

    def last(m, carry):
        recv_halo(hgrad_halo, m)

        @pl.when(m >= 2)
        def _():
            gf_copy(m - 2).wait()

        rows = jnp.concatenate([hgrad[e, m] for e in range(4)], axis=1)
        wide[...] = jnp.dot(rows, w_inner_back[...], preferred_element_type=F32)
        for o in range(2):
            total = (
                roll_rows(wide[:, lanes(o * 3)], -1)
                + wide[:, lanes(o * 3 + 1)]
                + roll_rows(wide[:, lanes(o * 3 + 2)], 1)
            )
            gf_buf[lax.rem(m, 2), o] = total.astype(BF16)
        gf_copy(m).start()

        for n in range(members):
            @pl.when(m == n)
            def _():
                inner_steps[n + 1]()
                if n > 0:
                    head_steps[n + 2]()
                if n == 0:
                    pass_on(hgrad_halo, members - 2)
                    pass_on(hgrad_halo, members - 1)

        return carry

    lax.fori_loop(0, members, last, 0)

    for m in range(members):
        drain_halo(feat_halo, m)
        drain_halo(part_halo, m)
        drain_halo(hgrad_halo, m)
    for t in range(chunks):
        drain_halo(gfield_halo, t)
    for m in range(max(members - 2, 0), members):
        gf_copy(m).wait()
    for ab in range(9):
        gh_out[ab] = hs_out[ab * VP:ab * VP + gh_out.shape[1]]
    inner_steps[5]()
    for ab in range(9):
        gi_out[ab] = is_out[ab * LANE:(ab + 1) * LANE]


def sum_scratch(rows):
    piece = rows // 2 // MEM
    return [
        pltpu.VMEM((rows, LANE), F32),
        pltpu.VMEM((rows, LANE), F32),
        pltpu.VMEM((rows // 2, LANE), F32),
        pltpu.VMEM((MEM, piece, LANE), BF16),
        pltpu.VMEM((MEM, piece, LANE), BF16),
        pltpu.VMEM((MEM, piece, LANE), BF16),
        pltpu.VMEM((2, MEM, piece, LANE), BF16),
    ]


def shards(features, conv_inner, conv_head, truth, kernel_width, var_weight):
    members, band, lon, channels = features.shape
    variables = conv_head.shape[3]
    lon_pad = -(-lon // (4 * LANE)) * 4 * LANE
    third = lon_pad // 4
    kin = conv_inner.reshape(9, channels, channels)
    ht = jnp.swapaxes(conv_head.reshape(9, channels, variables), 1, 2)
    width = kernel_width.reshape(1, variables)
    weight = var_weight.reshape(1, variables)

    any_spec = pl.BlockSpec(memory_space=pl.ANY)
    vmem = pl.BlockSpec(memory_space=pltpu.VMEM)
    dma = pltpu.SemaphoreType.DMA
    scratch = [
        pltpu.VMEM((4, members, lon_pad, LANE), BF16),
        pltpu.VMEM((lon, 6 * LANE), F32),
        pltpu.VMEM((members, lon_pad, 6 * LANE), BF16),
        pltpu.VMEM((members, lon, 2 * LANE), BF16),
        pltpu.VMEM((4, members, lon, LANE), BF16),
        pltpu.VMEM((6 * LANE, lon_pad), BF16),
        pltpu.VMEM((members, 2, VP, lon_pad), F32),
        pltpu.VMEM((MEM, members, VP, third), BF16),
        pltpu.VMEM((MEM, members, VP, third), BF16),
        pltpu.VMEM((MEM, members, VP, third), BF16),
        pltpu.VMEM((MEM, members, VP, third), BF16),
        pltpu.VMEM((members, 4, VP, lon_pad), BF16),
        pltpu.VMEM((4 * LANE, 6 * LANE), BF16),
        pltpu.VMEM((4 * VP, 6 * LANE), BF16),
        pltpu.VMEM((2 * LANE, 3 * LANE), BF16),
        pltpu.VMEM((4 * LANE, 6 * LANE), BF16),
        pltpu.VMEM((members, lon // 2, LANE), BF16),
        pltpu.VMEM((members, 2, VP, third), BF16),
        pltpu.VMEM((VP // 16, members // 2, 16, lon_pad), BF16),
        pltpu.VMEM((members, lon // 2, LANE), BF16),
        pltpu.VMEM((6 * LANE, 4 * LANE), F32),
        pltpu.VMEM((4 * VP, 6 * LANE), F32),
        pltpu.VMEM((2, 2, lon, LANE), BF16),
        pltpu.VMEM((3, VP, LANE), F32),
        pltpu.VMEM((VP, third), F32),
        *sum_scratch(HEAD_ROWS),
        *sum_scratch(9 * LANE),
        dma((members,)),
        dma((2, members)), dma((2, members)),
        dma((2, members)), dma((2, members)),
        dma((VP // 16,)), dma((VP // 16,)),
        dma((VP // 16,)), dma((VP // 16,)),
        dma((2, VP // 16)), dma((2, VP // 16)),
        dma((2, members)), dma((2, members)),
        dma((10,)), dma((10,)),
        dma((2,)),
        dma((4, VP // 16)), dma((4, VP // 16)),
    ]
    grad_features, inner, head = pl.pallas_call(
        whole_block,
        out_shape=(
            jax.ShapeDtypeStruct(features.shape, BF16),
            jax.ShapeDtypeStruct((9, channels, channels), F32),
            jax.ShapeDtypeStruct((9, variables, channels), F32),
        ),
        in_specs=[any_spec, vmem, vmem, vmem, vmem, vmem],
        out_specs=(any_spec, vmem, vmem),
        scratch_shapes=scratch,
        compiler_params=pltpu.CompilerParams(
            collective_id=0, has_side_effects=True, vmem_limit_bytes=67043328
        ),
    )(features, kin, ht, width, weight, truth)
    return (
        grad_features,
        inner.reshape(3, 3, channels, channels),
        jnp.swapaxes(head, 1, 2).reshape(3, 3, channels, variables),
    )


def solution(mesh):
    in_specs = (P("mem", "lat", None, None), P(), P(), P(None, "lat", None), P(), P())
    out_specs = (P("mem", "lat", None, None), P(), P())
    return jax.shard_map(shards, mesh=mesh, in_specs=in_specs, out_specs=out_specs, check_vma=False)
```

```python
import math
import jax
import jax.numpy as jnp
from jax import lax
from jax.experimental import pallas as pl
from jax.experimental.pallas import tpu as pltpu
from jax.sharding import PartitionSpec as P

MESH_ID = pl.DeviceIdType.MESH
F32 = jnp.float32
BF16 = jnp.bfloat16
LANE = 128
VP = 80
MEM = 8
LAT = 16
HEAD_ROWS = 768
RELAYS = (0, LAT - 1)
GELU_A = math.sqrt(2.0 / math.pi)
GELU_B = 0.044715


def roll_rows(values, shift):
    return pltpu.roll(values, shift % values.shape[0], 0)


def transposed(values):
    return jnp.transpose(values.astype(F32)).astype(BF16)


def whole_block(
    feat, kin, ht, width, weight, truth,
    gf_out, gi_out, gh_out,
    feat_rows, wide, shifted, slope, hgrad, hgrad_t, own_field,
    part_out, part_in, field_out, values_in, grad_field,
    w_inner, w_head, w_head_back, w_inner_back,
    feat_relay, part_relay, gfield_relay, hgrad_relay,
    inner_acc, head_acc, gf_buf, prm, target_buf,
    hs_in, hs_out, hs_r1, hs_r2, hs_r3, hs_sb, hs_db,
    is_in, is_out, is_r1, is_r2, is_r3, is_sb, is_db,
    load_sem, fh_s, fh_r, ph_s, ph_r, a2_s, a2_r, b2_s, b2_r, gh_s, gh_r, hh_s, hh_r,
    hsum_sems, isum_sems, out_sem, relay_s, relay_r,
):
    lon = feat.shape[2]
    lon_pad = grad_field.shape[3]
    members = feat.shape[0]
    third = lon_pad // 4
    d = lax.axis_index("mem")
    r = lax.axis_index("lat")
    has_up = r > 0
    has_down = r < LAT - 1
    above = lax.rem(r + LAT - 1, LAT)
    below = lax.rem(r + 1, LAT)
    half = lax.rem(r, 2)
    seat = r // 2

    def mem_peer(k):
        return lax.rem(d + k, MEM)

    def lat_peer(k):
        return lax.rem(seat + k, MEM) * 2 + half

    partner = r + 1 - 2 * half

    def remote(src, dst, ss, rs, **where):
        return pltpu.make_async_remote_copy(
            src_ref=src, dst_ref=dst, send_sem=ss, recv_sem=rs,
            device_id=where, device_id_type=MESH_ID,
        )

    barrier = pltpu.get_barrier_semaphore()
    for k in range(1, MEM):
        pl.semaphore_signal(barrier, inc=1, device_id={"mem": mem_peer(k)}, device_id_type=MESH_ID)
    for k in range(1, LAT):
        pl.semaphore_signal(
            barrier, inc=1, device_id={"lat": lax.rem(r + k, LAT)}, device_id_type=MESH_ID
        )

    def load(m, row):
        return pltpu.make_async_copy(
            feat.at[m, row], feat_rows.at[1 + row, m, pl.ds(0, lon)], load_sem.at[m]
        )

    for m in range(members):
        for row in range(2):
            load(m, row).start()

    pl.semaphore_wait(barrier, MEM - 1 + LAT - 1)

    mid_up = r == LAT // 2 - 1
    mid_down = r == LAT // 2
    relay_down = RELAYS[0]
    relay_up = RELAYS[1]
    is_relay = jnp.logical_or(r == relay_down, r == relay_up)
    relay_end = jnp.where(r == relay_down, LAT // 2, LAT // 2 - 1)
    part_rows = lon // 2

    def halo_rows(part):
        return pl.ds(0, lon) if part is None else pl.ds(part * part_rows, part_rows)

    def feat_ends(side, part, m):
        own, other = (1, 3) if side == 0 else (2, 0)
        return feat_rows.at[own, m, halo_rows(part)], feat_rows.at[other, m, halo_rows(part)]

    def part_ends(side, part, m):
        slots = pl.ds(side * 4, 4) if part is None else pl.ds(side * 4 + part * 2, 2)
        return part_out.at[slots, m], part_in.at[slots, m]

    def gfield_ends(side, part, t):
        own, other = (1, 3) if side == 0 else (2, 0)
        rows = pl.ds(pl.multiple_of(t * 16, 16), 16)
        which = pl.ds(0, members) if part is None else pl.ds(part * (members // 2), members // 2)
        return grad_field.at[which, own, rows], grad_field.at[which, other, rows]

    def hgrad_ends(side, part, m):
        own, other = (1, 3) if side == 0 else (2, 0)
        return hgrad.at[own, m, halo_rows(part)], hgrad.at[other, m, halo_rows(part)]

    feat_halo = (feat_ends, fh_s, fh_r, feat_relay, 0)
    part_halo = (part_ends, ph_s, ph_r, part_relay, 1)
    gfield_halo = (gfield_ends, gh_s, gh_r, gfield_relay, 2)
    hgrad_halo = (hgrad_ends, hh_s, hh_r, hgrad_relay, 3)

    sides = (
        (0, has_up, has_down, above, mid_down, relay_up),
        (1, has_down, has_up, below, mid_up, relay_down),
    )

    def direct(kind, side, part, m, where):
        ends, ss, rs, _, _ = kind
        src, dst = ends(side, part, m)
        return remote(src, dst, ss.at[side, m], rs.at[side, m], lat=where)

    def to_relay(kind, side, m, where):
        ends, ss, _, buffer, row = kind
        return remote(ends(side, 1, m)[0], buffer.at[m], ss.at[side, m], relay_r.at[row, m], lat=where)

    def from_relay(kind, side, m):
        ends, _, rs, buffer, row = kind
        return remote(
            buffer.at[m], ends(side, 1, m)[1], relay_s.at[row, m], rs.at[side, m], lat=relay_end
        )

    def send_halo(kind, m):
        for side, sends, _, where, by_relay, relay in sides:
            @pl.when(jnp.logical_and(sends, jnp.logical_not(by_relay)))
            def _():
                direct(kind, side, 0, m, where).start()
                direct(kind, side, 1, m, where).start()

            @pl.when(by_relay)
            def _():
                to_relay(kind, side, m, relay).start()
                direct(kind, side, 0, m, where).start()

    def recv_halo(kind, m):
        for side, _, receives, where, _, _ in sides:
            @pl.when(receives)
            def _():
                direct(kind, side, None, m, where).wait_recv()

    def drain_halo(kind, m):
        for side, sends, _, where, _, _ in sides:
            @pl.when(sends)
            def _():
                direct(kind, side, None, m, where).wait_send()

        for side, relay in ((0, relay_up), (1, relay_down)):
            @pl.when(r == relay)
            def _():
                from_relay(kind, side, m).wait_send()

    def pass_on(kind, m):
        for side, relay in ((0, relay_up), (1, relay_down)):
            @pl.when(r == relay)
            def _():
                to_relay(kind, side, m, relay_end).wait_recv()
                from_relay(kind, side, m).start()

    for m in range(members):
        pltpu.make_async_copy(
            feat.at[m], feat_rows.at[pl.ds(1, 2), m, pl.ds(0, lon)], load_sem.at[m]
        ).wait()
        send_halo(feat_halo, m)

    feat_rows[:, :, lon:, :] = jnp.zeros((4, members, lon_pad - lon, LANE), BF16)
    shifted[:, lon:, :] = jnp.zeros((members, lon_pad - lon, shifted.shape[2]), BF16)

    @pl.when(r == 0)
    def _():
        for m in range(members):
            feat_rows[0, m, 0:lon] = jnp.zeros((lon, LANE), BF16)
            hgrad[0, m] = jnp.zeros((lon, LANE), BF16)
            grad_field[m, 0] = jnp.zeros((VP, lon_pad), BF16)
            for q in range(4):
                part_in[4 + q, m] = jnp.zeros((VP, third), BF16)

    @pl.when(r == LAT - 1)
    def _():
        for m in range(members):
            feat_rows[3, m, 0:lon] = jnp.zeros((lon, LANE), BF16)
            hgrad[3, m] = jnp.zeros((lon, LANE), BF16)
            grad_field[m, 3] = jnp.zeros((VP, lon_pad), BF16)
            for q in range(4):
                part_in[q, m] = jnp.zeros((VP, third), BF16)

    w_inner[...] = jnp.zeros(w_inner.shape, BF16)
    w_inner_back[...] = jnp.zeros(w_inner_back.shape, BF16)
    w_head[...] = jnp.zeros(w_head.shape, BF16)
    w_head_back[...] = jnp.zeros(w_head_back.shape, BF16)
    for a in range(3):
        for b in range(3):
            block = kin[a * 3 + b]
            block_t = transposed(block)
            head_t = ht[a * 3 + b]
            nv = head_t.shape[0]
            for o in range(2):
                cols = slice((o * 3 + b) * LANE, (o * 3 + b + 1) * LANE)
                w_inner[(o + a) * LANE:(o + a + 1) * LANE, cols] = block
                e = o - a + 2
                w_inner_back[e * LANE:(e + 1) * LANE, cols] = block_t
                row = o - a + 2
                w_head[row * VP:row * VP + nv, b * 2 * LANE + o * LANE:b * 2 * LANE + (o + 1) * LANE] = head_t
            w_head_back[(2 - a) * VP:(2 - a) * VP + nv, b * LANE:(b + 1) * LANE] = head_t

    def column(ref, fill):
        nv = ref.shape[1]
        row = jnp.concatenate([ref[...], jnp.full((1, LANE - nv), fill, F32)], axis=1)
        return jnp.transpose(jnp.broadcast_to(row, (LANE, LANE)))[0:VP]

    widths = column(width, 1.0)
    inverse = 1.0 / (widths * widths)
    scaling = jnp.sqrt(0.5 * math.log2(math.e) * inverse)
    factor = column(weight, 0.0) * inverse / scaling
    prm[0] = scaling
    prm[1] = factor * (2.0 / (MEM * members - 1))
    prm[2] = factor * 2.0
    target_buf[...] = jnp.zeros(target_buf.shape, F32)
    for quarter in range(4):
        for row in range(2):
            @pl.when(d == row * 4 + quarter)
            def _():
                stop = min((quarter + 1) * third, lon)
                target_buf[0:truth.shape[0], 0:stop - quarter * third] = truth[:, row, quarter * third:stop]

    def lanes(index):
        return slice(index * LANE, (index + 1) * LANE)

    def forward(m):
        recv_halo(feat_halo, m)
        rows = jnp.concatenate([feat_rows[e, m, 0:lon] for e in range(4)], axis=1)
        wide[...] = jnp.dot(rows, w_inner[...], preferred_element_type=F32)
        for o in range(2):
            pre = (
                roll_rows(wide[:, lanes(o * 3)], 1)
                + wide[:, lanes(o * 3 + 1)]
                + roll_rows(wide[:, lanes(o * 3 + 2)], -1)
            )
            square = pre * pre
            th = jnp.tanh(GELU_A * pre * (1.0 + GELU_B * square))
            cdf = 0.5 + 0.5 * th
            hidden = pre * cdf
            grad = cdf + 0.5 * pre * (1.0 - th * th) * (GELU_A * (1.0 + 3.0 * GELU_B * square))
            slope[m, :, lanes(o)] = grad.astype(BF16)
            shifted[m, 0:lon, lanes(o)] = roll_rows(hidden, 1).astype(BF16)
            shifted[m, 0:lon, lanes(2 + o)] = hidden.astype(BF16)
            shifted[m, 0:lon, lanes(4 + o)] = roll_rows(hidden, -1).astype(BF16)
        slot = m
        for q in range(4):
            sums = lax.dot_general(
                w_head[...], shifted[m, q * third:(q + 1) * third, :],
                (((1,), (1,)), ((), ())), preferred_element_type=F32,
            )
            part_out[q, m] = sums[0:VP].astype(BF16)
            own_field[slot, 0, :, q * third:(q + 1) * third] = sums[VP:2 * VP]
            own_field[slot, 1, :, q * third:(q + 1) * third] = sums[2 * VP:3 * VP]
            part_out[4 + q, m] = sums[3 * VP:4 * VP].astype(BF16)
        send_halo(part_halo, m)

    chunks = VP // 16

    def tile(t):
        return pl.ds(t * 16 if isinstance(t, int) else pl.multiple_of(t * 16, 16), 16)

    def field_copy(m, t, k):
        p = mem_peer(k)
        return remote(
            field_out.at[p, m, tile(t)], values_in.at[d, m, tile(t)],
            a2_s.at[t], a2_r.at[t], mem=p,
        )

    def finish_field(m):
        recv_halo(part_halo, m)
        slot = m
        for row in range(2):
            for q in range(4):
                total = own_field[slot, row, :, q * third:(q + 1) * third] + part_in[
                    (1 - row) * 4 + q, m
                ].astype(F32)
                field_out[row * 4 + q, m] = total.astype(BF16)
        early = members // 2

        @pl.when(m < early)
        def _():
            for t in range(chunks):
                for k in range(1, MEM):
                    field_copy(m, t, k).start()

        @pl.when(m == members - 1)
        def _():
            for t in range(chunks):
                for late in range(early, members):
                    for k in range(1, MEM):
                        field_copy(late, t, k).start()

        values_in[d, m] = field_out[d, m]

    pass_on(feat_halo, 0)
    pass_on(feat_halo, 1)

    def forward_step(m, carry):
        forward(m)

        @pl.when(m == 0)
        def _():
            for n in range(2, members):
                pass_on(feat_halo, n)

        @pl.when(m > 0)
        def _():
            pass_on(part_halo, m - 1)

        return carry

    def finish_step(m, carry):
        finish_field(m)
        return carry

    lax.fori_loop(0, members, forward_step, 0)
    pass_on(part_halo, members - 1)
    lax.fori_loop(0, members, finish_step, 0)

    grad_out = field_out
    count = MEM * members
    own_row = 1 + d // 4
    own_lane = lax.rem(d, 4) * third

    def place(j):
        return slice((j // 2) * 16, (j // 2 + 1) * 16), slice((j % 2) * third, (j % 2 + 1) * third)

    def back_copy(t, k):
        p = mem_peer(k)
        rows = tile(t)
        return remote(
            grad_out.at[p, :, rows],
            grad_field.at[:, own_row, rows, pl.ds(pl.multiple_of(own_lane, LANE), third)],
            b2_s.at[t], b2_r.at[t], mem=p,
        )

    block = 8
    lane_groups = third // LANE
    used_groups = -(-truth.shape[0] // 8)

    def pair_chunk(t, carry):
        rows16 = tile(t)

        others = pl.ds(0, MEM - 1)
        remote(
            field_out.at[others, :, rows16], values_in.at[others, :, rows16],
            a2_s.at[t], a2_r.at[t], mem=mem_peer(1),
        ).wait()
        scale = jnp.concatenate([prm[0, rows16]] * lane_groups, axis=1)
        for j in range(count):
            rows, cols = place(j)
            wide[rows, cols] = values_in[j // members, j % members, rows16].astype(F32) * scale

        def group(unit, inner):
            sub = unit // lane_groups
            lane = lax.rem(unit, lane_groups) * LANE

            def at(j):
                return (
                    pl.ds(pl.multiple_of((j // 2) * 16 + sub * 8, 8), 8),
                    pl.ds(pl.multiple_of((j % 2) * third + lane, LANE), LANE),
                )

            rows8 = pl.ds(pl.multiple_of(t * 16 + sub * 8, 8), 8)
            target = target_buf[rows8, pl.ds(pl.multiple_of(lane, LANE), LANE)] * prm[0, rows8]
            pair_weight = prm[1, rows8]
            truth_weight = prm[2, rows8]

            def term(x, y):
                u = x - y
                return u * jnp.exp2(u * (y - x))

            for i0 in range(0, count, block):
                xi = [wide[at(i0 + i)] for i in range(block)]
                sums = [None] * block
                for i in range(block):
                    for j in range(i + 1, block):
                        w = term(xi[j], xi[i])
                        sums[i] = w if sums[i] is None else sums[i] + w
                        sums[j] = -w if sums[j] is None else sums[j] - w
                if i0 > 0:
                    sums = [s + wide[at(count + i0 + i)] for i, s in enumerate(sums)]
                for j0 in range(i0 + block, count, block):
                    xj = [wide[at(j0 + j)] for j in range(block)]
                    back = [None] * block
                    for j in range(block):
                        for i in range(block):
                            w = term(xj[j], xi[i])
                            sums[i] = sums[i] + w
                            back[j] = -w if back[j] is None else back[j] - w
                    for j in range(block):
                        old = back[j] if i0 == 0 else wide[at(count + j0 + j)] + back[j]
                        wide[at(count + j0 + j)] = old
                for i in range(block):
                    near = term(xi[i], target)
                    wide[at(count + i0 + i)] = pair_weight * sums[i] + truth_weight * near
            return inner

        subs = jnp.minimum(2, used_groups - 2 * t)
        lax.fori_loop(0, subs * lane_groups, group, 0)
        keep = lax.broadcasted_iota(jnp.int32, (16, third), 0) < subs * 8
        for j in range(count):
            rows, cols = place(count + j)
            grad_out[j // members, j % members, rows16] = jnp.where(keep, wide[rows, cols], 0.0).astype(BF16)
        for k in range(1, MEM):
            back_copy(t, k).start()
        grad_field[:, own_row, rows16, pl.ds(pl.multiple_of(own_lane, LANE), third)] = grad_out[d, :, rows16]
        return carry

    lax.fori_loop(0, chunks, pair_chunk, 0)

    def wait_back(t, carry):
        pass_on(gfield_halo, t)
        others = pl.ds(0, MEM - 1)
        remote(
            grad_out.at[others, :, tile(t)], values_in.at[others, :, tile(t)],
            b2_s.at[t], b2_r.at[t], mem=mem_peer(1),
        ).wait()
        send_halo(gfield_halo, t)
        return carry

    lax.fori_loop(0, chunks, wait_back, 0)

    inner_acc[...] = jnp.zeros(inner_acc.shape, F32)
    head_acc[...] = jnp.zeros(head_acc.shape, F32)

    def at_rows(start, size):
        return pl.ds(pl.multiple_of(start, 8), size)

    def device_sum(src, dst, r1, r2, r3, sb, db, sems):
        half_rows = src.shape[0] // 2
        piece_rows = half_rows // MEM
        my_half = half * half_rows
        my_piece = my_half + d * piece_rows

        def scatter_pair():
            return remote(
                src.at[at_rows((1 - half) * half_rows, half_rows)], r1, sems.at[0], sems.at[1], lat=partner
            )

        def scatter(k):
            return remote(
                sb.at[mem_peer(k)], r2.at[k], sems.at[2], sems.at[3], mem=mem_peer(k),
            )

        def share(k):
            return remote(r3.at[seat], r3.at[seat], sems.at[4], sems.at[5], lat=lat_peer(k))

        def gather(k):
            piece = db.at[half, d]
            return remote(piece, piece, sems.at[6], sems.at[7], mem=mem_peer(k))

        def gather_pair():
            piece = db.at[half]
            return remote(piece, piece, sems.at[8], sems.at[9], lat=partner)

        def each(copy_of, act):
            for k in range(1, MEM):
                act(copy_of(k))

        start = lambda c: c.start()

        def wait_all(n, buffer, where):
            slabs = buffer.at[pl.ds(0, MEM - 1)]
            remote(slabs, slabs, sems.at[2 * n], sems.at[2 * n + 1], **where).wait()

        def step_0():
            scatter_pair().start()

        def step_1():
            scatter_pair().wait()
            mine = at_rows(my_half, half_rows)
            src[mine] = src[mine] + r1[...]
            for p in range(MEM):
                sb[p] = src[at_rows(my_half + p * piece_rows, piece_rows)].astype(BF16)
            each(scatter, start)

        def step_2():
            wait_all(1, r2, {"mem": mem_peer(1)})
            mine = at_rows(my_piece, piece_rows)
            total = src[mine]
            for k in range(1, MEM):
                total = total + r2[k].astype(F32)
            r3[seat] = total.astype(BF16)
            each(share, start)

        def step_3():
            wait_all(2, r3, {"lat": lat_peer(1)})
            total = r3[0].astype(F32)
            for k in range(1, MEM):
                total = total + r3[k].astype(F32)
            db[half, d] = (total * (1.0 / (2 * LAT * lon))).astype(BF16)
            each(gather, start)

        def step_4():
            wait_all(3, db.at[0], {"mem": mem_peer(1)})
            gather_pair().start()

        def step_5():
            gather_pair().wait()
            for h in range(2):
                for p in range(MEM):
                    start_row = h * half_rows + p * piece_rows
                    dst[start_row:start_row + piece_rows] = db[h, p].astype(F32)

        return step_0, step_1, step_2, step_3, step_4, step_5

    head_steps = device_sum(hs_in, hs_out, hs_r1, hs_r2, hs_r3, hs_sb, hs_db, hsum_sems)
    inner_steps = device_sum(is_in, is_out, is_r1, is_r2, is_r3, is_sb, is_db, isum_sems)

    def head_gradient(m, carry):
        fields = grad_field[m].reshape(4 * VP, lon_pad)
        head_acc[...] += jnp.dot(fields, shifted[m], preferred_element_type=F32)
        return carry

    def halo_tiles(t, carry):
        recv_halo(gfield_halo, t)
        return carry

    lax.fori_loop(0, chunks, halo_tiles, 0)
    lax.fori_loop(0, members, head_gradient, 0)
    for a in range(3):
        for b in range(3):
            base = (a * 3 + b) * VP
            hs_in[base:base + VP] = (
                head_acc[(2 - a) * VP:(3 - a) * VP, lanes(b * 2)]
                + head_acc[(3 - a) * VP:(4 - a) * VP, lanes(b * 2 + 1)]
            )
    hs_in[9 * VP:] = jnp.zeros((hs_in.shape[0] - 9 * VP, LANE), F32)
    head_steps[0]()

    def backward(m, carry):
        for i in range(2):
            stack = [grad_field[m, i + j] for j in range(3)]
            stack.append(jnp.zeros((2 * LANE - 3 * VP, lon_pad), BF16))
            columns = transposed(jnp.concatenate(stack, axis=0))
            wide[:, 0:3 * LANE] = jnp.dot(
                columns[0:lon], w_head_back[...], preferred_element_type=F32
            )
            total = (
                roll_rows(wide[:, lanes(0)], -1) + wide[:, lanes(1)] + roll_rows(wide[:, lanes(2)], 1)
            )
            hg = total * slope[m, :, lanes(i)].astype(F32)
            hgrad[1 + i, m] = hg.astype(BF16)
            tail = jnp.zeros((lon_pad - lon, LANE), F32)
            for b in range(3):
                moved = hg if b == 1 else roll_rows(hg, b - 1)
                hgrad_t[(i * 3 + b) * LANE:(i * 3 + b + 1) * LANE, :] = jnp.transpose(
                    jnp.concatenate([moved, tail], axis=0)
                ).astype(BF16)
        send_halo(hgrad_halo, m)
        rows = jnp.concatenate([feat_rows[e, m] for e in range(4)], axis=1)
        inner_acc[...] += jnp.dot(hgrad_t[...], rows, preferred_element_type=F32)
        @pl.when(m >= 2)
        def _():
            pass_on(hgrad_halo, m - 2)

        for n in (1, 2):
            @pl.when(m == 2 * n - 1)
            def _():
                head_steps[n]()

        return carry

    lax.fori_loop(0, members, backward, 0)
    for a in range(3):
        for b in range(3):
            ab = a * 3 + b
            is_in[ab * LANE:(ab + 1) * LANE] = jnp.transpose(
                inner_acc[b * LANE:(b + 1) * LANE, lanes(a)]
                + inner_acc[(3 + b) * LANE:(4 + b) * LANE, lanes(1 + a)]
            )

    def gf_copy(m):
        return pltpu.make_async_copy(gf_buf.at[lax.rem(m, 2)], gf_out.at[m], out_sem.at[lax.rem(m, 2)])

    inner_steps[0]()

    def last(m, carry):
        recv_halo(hgrad_halo, m)

        @pl.when(m >= 2)
        def _():
            gf_copy(m - 2).wait()

        rows = jnp.concatenate([hgrad[e, m] for e in range(4)], axis=1)
        wide[...] = jnp.dot(rows, w_inner_back[...], preferred_element_type=F32)
        for o in range(2):
            total = (
                roll_rows(wide[:, lanes(o * 3)], -1)
                + wide[:, lanes(o * 3 + 1)]
                + roll_rows(wide[:, lanes(o * 3 + 2)], 1)
            )
            gf_buf[lax.rem(m, 2), o] = total.astype(BF16)
        gf_copy(m).start()

        for n in range(members):
            @pl.when(m == n)
            def _():
                inner_steps[n + 1]()
                if n > 0:
                    head_steps[n + 2]()
                if n == 0:
                    pass_on(hgrad_halo, members - 2)
                    pass_on(hgrad_halo, members - 1)

        return carry

    lax.fori_loop(0, members, last, 0)

    for m in range(members):
        drain_halo(feat_halo, m)
        drain_halo(part_halo, m)
        drain_halo(hgrad_halo, m)
    for t in range(chunks):
        drain_halo(gfield_halo, t)
    for m in range(max(members - 2, 0), members):
        gf_copy(m).wait()
    for ab in range(9):
        gh_out[ab] = hs_out[ab * VP:ab * VP + gh_out.shape[1]]
    inner_steps[5]()
    for ab in range(9):
        gi_out[ab] = is_out[ab * LANE:(ab + 1) * LANE]


def sum_scratch(rows):
    piece = rows // 2 // MEM
    return [
        pltpu.VMEM((rows, LANE), F32),
        pltpu.VMEM((rows, LANE), F32),
        pltpu.VMEM((rows // 2, LANE), F32),
        pltpu.VMEM((MEM, piece, LANE), BF16),
        pltpu.VMEM((MEM, piece, LANE), BF16),
        pltpu.VMEM((MEM, piece, LANE), BF16),
        pltpu.VMEM((2, MEM, piece, LANE), BF16),
    ]


def shards(features, conv_inner, conv_head, truth, kernel_width, var_weight):
    members, band, lon, channels = features.shape
    variables = conv_head.shape[3]
    lon_pad = -(-lon // (4 * LANE)) * 4 * LANE
    third = lon_pad // 4
    kin = conv_inner.reshape(9, channels, channels)
    ht = jnp.swapaxes(conv_head.reshape(9, channels, variables), 1, 2)
    width = kernel_width.reshape(1, variables)
    weight = var_weight.reshape(1, variables)

    any_spec = pl.BlockSpec(memory_space=pl.ANY)
    vmem = pl.BlockSpec(memory_space=pltpu.VMEM)
    dma = pltpu.SemaphoreType.DMA
    scratch = [
        pltpu.VMEM((4, members, lon_pad, LANE), BF16),
        pltpu.VMEM((lon, 6 * LANE), F32),
        pltpu.VMEM((members, lon_pad, 6 * LANE), BF16),
        pltpu.VMEM((members, lon, 2 * LANE), BF16),
        pltpu.VMEM((4, members, lon, LANE), BF16),
        pltpu.VMEM((6 * LANE, lon_pad), BF16),
        pltpu.VMEM((members, 2, VP, lon_pad), F32),
        pltpu.VMEM((MEM, members, VP, third), BF16),
        pltpu.VMEM((MEM, members, VP, third), BF16),
        pltpu.VMEM((MEM, members, VP, third), BF16),
        pltpu.VMEM((MEM, members, VP, third), BF16),
        pltpu.VMEM((members, 4, VP, lon_pad), BF16),
        pltpu.VMEM((4 * LANE, 6 * LANE), BF16),
        pltpu.VMEM((4 * VP, 6 * LANE), BF16),
        pltpu.VMEM((2 * LANE, 3 * LANE), BF16),
        pltpu.VMEM((4 * LANE, 6 * LANE), BF16),
        pltpu.VMEM((members, lon // 2, LANE), BF16),
        pltpu.VMEM((members, 2, VP, third), BF16),
        pltpu.VMEM((VP // 16, members // 2, 16, lon_pad), BF16),
        pltpu.VMEM((members, lon // 2, LANE), BF16),
        pltpu.VMEM((6 * LANE, 4 * LANE), F32),
        pltpu.VMEM((4 * VP, 6 * LANE), F32),
        pltpu.VMEM((2, 2, lon, LANE), BF16),
        pltpu.VMEM((3, VP, LANE), F32),
        pltpu.VMEM((VP, third), F32),
        *sum_scratch(HEAD_ROWS),
        *sum_scratch(9 * LANE),
        dma((members,)),
        dma((2, members)), dma((2, members)),
        dma((2, members)), dma((2, members)),
        dma((VP // 16,)), dma((VP // 16,)),
        dma((VP // 16,)), dma((VP // 16,)),
        dma((2, VP // 16)), dma((2, VP // 16)),
        dma((2, members)), dma((2, members)),
        dma((10,)), dma((10,)),
        dma((2,)),
        dma((4, VP // 16)), dma((4, VP // 16)),
    ]
    grad_features, inner, head = pl.pallas_call(
        whole_block,
        out_shape=(
            jax.ShapeDtypeStruct(features.shape, BF16),
            jax.ShapeDtypeStruct((9, channels, channels), F32),
            jax.ShapeDtypeStruct((9, variables, channels), F32),
        ),
        in_specs=[any_spec, vmem, vmem, vmem, vmem, vmem],
        out_specs=(any_spec, vmem, vmem),
        scratch_shapes=scratch,
        compiler_params=pltpu.CompilerParams(
            collective_id=0, has_side_effects=True, vmem_limit_bytes=67043328
        ),
    )(features, kin, ht, width, weight, truth)
    return (
        grad_features,
        inner.reshape(3, 3, channels, channels),
        jnp.swapaxes(head, 1, 2).reshape(3, 3, channels, variables),
    )


def solution(mesh):
    in_specs = (P("mem", "lat", None, None), P(), P(), P(None, "lat", None), P(), P())
    out_specs = (P("mem", "lat", None, None), P(), P())
    return jax.shard_map(shards, mesh=mesh, in_specs=in_specs, out_specs=out_specs, check_vma=False)
```
